256 devices in a mesh: groups: 2 (over y), seq: 64 (over x, z), width: 2 (over core).
Axes of the slice: x: 4, y: 2, z: 16, core: 2. Of those that a mesh axis runs over, the one named last changes fastest.
The devices are a block of a 4x16x16 slice.
Arguments:
- span_tokens: bfloat16 [4096, 16384], P(('groups', 'seq'), 'width'), parts along dimension 0, may hold values from -6 to 6
- kv_weight: bfloat16 [16384, 1024], P('seq', 'width'), may hold values from -0.046875 to 0.046875
- query_weight: bfloat16 [16384, 8192], P('seq', 'width'), may hold values from -0.046875 to 0.046875
- out_weight: bfloat16 [8192, 16384], P('width', 'seq'), may hold values from -6 to 6
- cache_keys: bfloat16 [131072, 4, 128], P(('groups', 'seq'), 'width'), parts along dimension 0, may hold values from -1000 to 1000
- cache_values: bfloat16 [131072, 4, 128], P(('groups', 'seq'), 'width'), parts along dimension 0, may hold values from -6 to 6
- hidden: bfloat16 [2, 64, 16384], P(None, 'groups', 'seq'), parts along dimension 1, may hold values from -6 to 6
- lengths: int32 [64], P('groups'), parts along dimension 0, may hold values from 1 to 65536
- offset: int32 [2], P('groups'), parts along dimension 0, may hold values from 32768 to 65536
Outputs:
- span_kv: bfloat16 [4096, 1024], P(('groups', 'seq'), 'width'), parts along dimension 0
- attended: bfloat16 [2, 64, 16384], P(None, 'groups', ('seq', 'width')), parts along dimension 1
The draws below stay inside these ranges and needn't reach their ends.
There are 2 independent parts, one for each index of `groups`. The reference program is written for one: setup_inputs(seed, part) draws one part's arguments, and reference() takes and returns one part's arrays. A program takes and returns all parts, laid end to end along the dimension named above; an argument that names none is the same for every part. Nothing has to cross between parts.
All inputs are finite; a program needn't handle non-finite values.
Results may differ from the reference program's by a relative error of at most 0.014.
The reference program's roundings to bfloat16 on the way count: a program that leaves them out, or rounds other values in their place, can miss the bound.
Values may be sent and summed in bfloat16 or wider, within the bound.
No kernel may reach another device: no remote copies, remote signals or barrier semaphores. Data moves between devices by JAX's collectives and lax.ppermute only.
A program may use at most 128 MiB of HBM per device.

```python
import math
import jax
import jax.numpy as jnp
from jax import lax

D = 16384
HD = 128
QH = 64
KVH = 4
STEPS = 2
BRANCHES = 32
TOK_DEV = 32
KEY_BLOCK = 256
SPAN = 2048
CACHE = 65536


def draw_cache_keys(key, part):
    extent = (CACHE, KVH, HD)
    drawn = jax.random.normal(jax.random.fold_in(key, 11), extent, jnp.float32)
    return drawn.astype(jnp.bfloat16)


def plant(entries, rng, low, top_value):
    place = [jax.random.randint(jax.random.fold_in(rng, axis), (), 0, length) for axis, length in enumerate(entries.shape)]
    widest = entries.shape.index(max(entries.shape))
    beside = place[:widest] + [(place[widest] + 1) % entries.shape[widest]] + place[widest + 1:]
    return entries.at[tuple(place)].set(low).at[tuple(beside)].set(top_value)


def level_of(own_key, shape, shards, least, largest):
    level = 1.0
    for position, blocks in shards:
        heights = jax.random.uniform(jax.random.fold_in(jax.random.fold_in(own_key, 6), position), (blocks,), jnp.float32, least / len(shards), largest / len(shards))
        level = level * jnp.repeat(jnp.exp(heights), shape[position] // blocks).reshape((-1,) + (1,) * (len(shape) - 1 - position))
    return level


def normal_values(rng, shape, deviation, bound, cuts=(), held_as=jnp.bfloat16):
    factor_of = level_of(rng, shape, cuts, -0.22, 0.18) if cuts else 1.0
    values = jax.random.normal(rng, shape, jnp.float32) * deviation * factor_of
    return jnp.minimum(jnp.maximum(values, -bound), bound).astype(held_as)


def setup_inputs(seed: int = 0, part: int = 0) -> dict:
    seeds = jax.random.split(jax.random.key(seed), 10)
    part_splits = jax.random.split(jax.random.fold_in(seeds[9], part), 10)
    span_tokens = normal_values(part_splits[0], (SPAN, D), 1.0, 6.0, ((0, 64), (1, 2)))
    kv_weight = normal_values(seeds[1], (D, 2 * KVH * HD), D ** -0.5, 0.046875, ((0, 64), (1, 2)))
    query_weight = normal_values(seeds[2], (D, QH * HD), D ** -0.5, 0.046875, ((0, 64), (1, 2)))
    out_weight = normal_values(seeds[3], (QH * HD, D), 1.0, 6.0, ((0, 2), (1, 64)))
    cache_keys = draw_cache_keys(jax.random.fold_in(jax.random.fold_in(seeds[9], part), 71), part)
    cache_values = normal_values(part_splits[5], (CACHE, KVH, HD), 1.0, 6.0, ((0, 64), (1, 2)))
    hidden = normal_values(part_splits[6], (STEPS, BRANCHES, D), 1.0, 6.0, ((2, 64),))
    lengths = plant(jax.random.randint(part_splits[7], (BRANCHES,), 1, CACHE + 1), jax.random.fold_in(part_splits[7], 1), 1, CACHE).astype(jnp.int32)
    offset = jax.random.randint(part_splits[8], (1,), CACHE // 2, CACHE + 1).astype(jnp.int32)
    return {"span_tokens": span_tokens, "kv_weight": kv_weight, "query_weight": query_weight, "out_weight": out_weight, "cache_keys": cache_keys, "cache_values": cache_values, "hidden": hidden, "lengths": lengths, "offset": offset}


MASKED_SCORE = -1e+30

def combine(earlier, later):
    highest = jnp.maximum(earlier[0], later[0])
    keep_a = jnp.exp(earlier[0] - highest)
    keep_b = jnp.exp(later[0] - highest)
    return (highest, earlier[1] * keep_a + later[1] * keep_b, earlier[2] * keep_a[..., None] + later[2] * keep_b[..., None])

def weigh_block(scores, allowed):
    masked = jnp.where(allowed, scores, MASKED_SCORE)
    highest = lax.optimization_barrier(jnp.max(masked, axis=-1))
    weights = jnp.where(allowed, jnp.exp(masked - highest[..., None]), 0.0)
    return (highest, lax.optimization_barrier(jnp.sum(weights, axis=-1)), weights.astype(jnp.bfloat16))

def shared_block(queries, key_block, value_block, allowed, factor):
    scores = jnp.einsum('hqd,khd->hqk', queries, key_block.astype(jnp.float32)) * factor
    highest, weight_sum, weights = weigh_block(scores, allowed)
    summed = jnp.einsum('hqk,khd->hqd', weights.astype(jnp.float32), value_block.astype(jnp.float32))
    return (highest, weight_sum, summed)

def reference(span_tokens, kv_weight, query_weight, out_weight, cache_keys, cache_values, hidden, lengths, offset):
    factor = 1.0 / math.sqrt(HD)
    grouped = QH // KVH
    row_count = STEPS * BRANCHES
    flat_rows = row_count * grouped
    span_kv = jnp.dot(span_tokens, kv_weight, preferred_element_type=jnp.float32).astype(jnp.bfloat16)
    states = hidden.reshape(row_count, D)
    query_rows = jnp.dot(states, query_weight, preferred_element_type=jnp.float32).astype(jnp.bfloat16)
    fresh_rows = jnp.dot(states, kv_weight, preferred_element_type=jnp.float32).astype(jnp.bfloat16)
    queries = query_rows.reshape(row_count, KVH, grouped, HD).transpose(1, 0, 2, 3).reshape(KVH, flat_rows, HD)
    queries = queries.astype(jnp.float32)
    visible = jnp.minimum(lengths, offset[0])
    visible_flat = jnp.repeat(jnp.tile(visible, STEPS), grouped)
    start_state = (jnp.full((KVH, flat_rows), MASKED_SCORE, jnp.float32), jnp.zeros((KVH, flat_rows), jnp.float32), jnp.zeros((KVH, flat_rows, HD), jnp.float32))

    def cache_step(running, block_id):
        leading = block_id * KEY_BLOCK
        key_block = lax.dynamic_slice_in_dim(cache_keys, leading, KEY_BLOCK, 0)
        value_block = lax.dynamic_slice_in_dim(cache_values, leading, KEY_BLOCK, 0)
        places = leading + jnp.arange(KEY_BLOCK, dtype=jnp.int32)
        allowed = (places[None, :] < visible_flat[:, None])[None]
        return (combine(running, shared_block(queries, key_block, value_block, allowed, factor)), None)
    running, unused = lax.scan(cache_step, start_state, jnp.arange(CACHE // KEY_BLOCK, dtype=jnp.int32))
    span_pairs = span_kv.reshape(SPAN, KVH, 2, HD)
    everywhere = jnp.ones((1, 1, 1), jnp.bool_)

    def span_step(running, block_id):
        leading = block_id * TOK_DEV
        pairs = lax.dynamic_slice_in_dim(span_pairs, leading, TOK_DEV, 0)
        return (combine(running, shared_block(queries, pairs[:, :, 0], pairs[:, :, 1], everywhere, factor)), None)
    running, unused = lax.scan(span_step, running, jnp.arange(SPAN // TOK_DEV, dtype=jnp.int32))
    grid = query_rows.reshape(STEPS, BRANCHES, KVH, grouped, HD).astype(jnp.float32)
    fresh_pairs = fresh_rows.reshape(STEPS, BRANCHES, KVH, 2, HD).astype(jnp.float32)
    self_scores = jnp.einsum('tbhgd,ubhd->htbgu', grid, fresh_pairs[:, :, :, 0]) * factor
    self_scores = self_scores.reshape(KVH, flat_rows, STEPS)
    causal = jnp.arange(STEPS)[None, :] <= jnp.arange(STEPS)[:, None]
    allowed = jnp.broadcast_to(causal[:, None, None, :], (STEPS, BRANCHES, grouped, STEPS)).reshape(flat_rows, STEPS)[None]
    highest, weight_sum, weights = weigh_block(self_scores, allowed)
    weights = weights.reshape(KVH, STEPS, BRANCHES, grouped, STEPS).astype(jnp.float32)
    summed = jnp.einsum('htbgu,ubhd->htbgd', weights, fresh_pairs[:, :, :, 1]).reshape(KVH, flat_rows, HD)
    finished = combine(running, (highest, weight_sum, summed))
    attention = (finished[2] / finished[1][..., None]).astype(jnp.bfloat16)
    attention = attention.reshape(KVH, row_count, grouped, HD).transpose(1, 0, 2, 3).reshape(row_count, QH * HD)
    attended = jnp.dot(attention, out_weight, preferred_element_type=jnp.float32).astype(jnp.bfloat16)
    return (span_kv, attended.reshape(STEPS, BRANCHES, D))
```

```python
import math

import jax
import jax.numpy as jnp
from jax import lax
from jax.experimental import pallas as pl
from jax.experimental.pallas import tpu as pltpu
from jax.sharding import Mesh
from jax.sharding import PartitionSpec as P

HD = 128
QH = 64
KVH = 4
SEQ = ("x", "z")
GROUPS_SEQ = ("groups", "x", "z")
SEQ_WIDTH = ("x", "z", "width")
MASKED_SCORE = -1e30
LOG2E = 1.4426950408889634
F32 = jnp.float32
BF16 = jnp.bfloat16


def exchanged(pieces, axis):
    return lax.all_to_all(pieces, axis, split_axis=0, concat_axis=0, tiled=True)


def copies_from(x, axis):
    return exchanged(jnp.broadcast_to(x, (lax.axis_size(axis), *x.shape)), axis)


def dot_f32(a, b):
    return jnp.dot(a, b, preferred_element_type=F32)


def project_body(states_ref, query_ref, fresh_ref, out_ref):
    states = states_ref[...]
    columns = query_ref.shape[1]
    out_ref[0, :, :columns] = dot_f32(states, query_ref[...])
    out_ref[0, :, columns:] = dot_f32(states, fresh_ref[...])


def project(states, query_weight, kv_weight, pieces):
    rows, depth = states.shape
    columns = query_weight.shape[1] // pieces
    extra = kv_weight.shape[1] // pieces
    return pl.pallas_call(
        project_body,
        grid=(pieces,),
        in_specs=[
            pl.BlockSpec((rows, depth), lambda c: (0, 0)),
            pl.BlockSpec((depth, columns), lambda c: (0, c)),
            pl.BlockSpec((depth, extra), lambda c: (0, c)),
        ],
        out_specs=pl.BlockSpec((1, rows, columns + extra), lambda c: (c, 0, 0)),
        out_shape=jax.ShapeDtypeStruct((pieces, rows, columns + extra), F32),
        name="project",
    )(states, query_weight, kv_weight)


def three_parts(x):
    high = x.astype(BF16).astype(F32)
    rest = x - high
    middle = rest.astype(BF16).astype(F32)
    return (high, middle, rest - middle)


def put_stats(lane, stats, head, heads, highest, total):
    for place, value in enumerate((*three_parts(highest), *three_parts(total))):
        stats = jnp.where(lane == place * heads + head, value, stats)
    return stats


def joined_stats(tail, heads):
    lanes = tail.shape[-1]
    whole = (
        tail + pltpu.roll(tail, lanes - heads, 1) + pltpu.roll(tail, lanes - 2 * heads, 1)
    )
    return whole, pltpu.roll(whole, lanes - 3 * heads, 1)


def split_stats(lane, highest, total, heads):
    parts = (*three_parts(highest), *three_parts(total))
    stats = jnp.where(lane < heads, parts[0], 0.0)
    for place in range(1, 6):
        here = (lane >= place * heads) & (lane < (place + 1) * heads)
        stats = jnp.where(here, pltpu.roll(parts[place], place * heads, 1), stats)
    return stats


def attend_body(q_ref, keys_ref, values_ref, span_ref, bias_ref, out_ref, k_ref, v_ref, *, scale):
    slots = keys_ref.shape[1]
    span = span_ref.shape[0]
    rows = q_ref.shape[1]
    heads = (q_ref.shape[2] - HD) // HD
    per_dot = 4
    total_keys = k_ref.shape[0]
    blank = jnp.zeros((total_keys - slots - span - rows, HD), BF16)
    k_ref[:slots, :] = keys_ref[0]
    v_ref[:slots, :] = values_ref[0]
    at = heads * HD
    k_ref[slots:, :] = jnp.concatenate([span_ref[:, :HD], q_ref[0, :, at:], blank], axis=0)
    v_ref[slots:, :] = jnp.concatenate([span_ref[:, HD:], q_ref[1, :, at:], blank], axis=0)
    bias = bias_ref[...]
    lane = lax.broadcasted_iota(jnp.int32, (rows, HD), 1)
    for piece in range(2):
        stats = jnp.zeros((rows, HD), F32)
        for first in range(0, heads, per_dot):
            q = jnp.concatenate(
                [
                    q_ref[piece, :, (first + i) * HD : (first + i + 1) * HD]
                    for i in range(per_dot)
                ],
                axis=0,
            )
            scores = lax.dot_general(
                q, k_ref[...], (((1,), (1,)), ((), ())), preferred_element_type=F32
            )
            scores = scores.reshape(per_dot, rows, total_keys) * scale + bias[None]
            highest = jnp.max(scores, axis=-1, keepdims=True)
            weights = jnp.exp2(scores - highest)
            total = jnp.sum(weights, axis=-1, keepdims=True)
            summed = dot_f32(
                weights.reshape(per_dot * rows, total_keys).astype(BF16), v_ref[...]
            )
            for i in range(per_dot):
                head = first + i
                out_ref[piece, :, head * HD : (head + 1) * HD] = summed[
                    i * rows : (i + 1) * rows
                ].astype(BF16)
                stats = put_stats(lane, stats, head, heads, highest[i], total[i])
        out_ref[piece, :, at:] = stats.astype(BF16)


def attend(projected, keys, values, span_kv, bias, scale):
    pieces, rows, width = projected.shape
    local_heads, slots, _ = keys.shape
    span = span_kv.shape[0]
    per_head = pieces // local_heads
    total_keys = bias.shape[1]
    body = lambda *refs: attend_body(*refs, scale=scale)
    return pl.pallas_call(
        body,
        grid=(local_heads,),
        in_specs=[
            pl.BlockSpec((per_head, rows, width), lambda h: (h, 0, 0)),
            pl.BlockSpec((1, slots, HD), lambda h: (h, 0, 0)),
            pl.BlockSpec((1, slots, HD), lambda h: (h, 0, 0)),
            pl.BlockSpec((span, 2 * HD), lambda h: (0, h)),
            pl.BlockSpec((rows, total_keys), lambda h: (0, 0)),
        ],
        out_specs=pl.BlockSpec((per_head, rows, width), lambda h: (h, 0, 0)),
        out_shape=jax.ShapeDtypeStruct((pieces, rows, width), BF16),
        scratch_shapes=[pltpu.VMEM((total_keys, HD), BF16), pltpu.VMEM((total_keys, HD), BF16)],
        name="attend",
    )(projected, keys, values, span_kv, bias)


def fold_body(in_ref, out_ref):
    sources, rows, width = in_ref.shape
    heads = (width - HD) // HD
    at = heads * HD
    lane = lax.broadcasted_iota(jnp.int32, (rows, HD), 1)
    stats = [joined_stats(in_ref[s, :, at:].astype(F32), heads) for s in range(sources)]
    highest = stats[0][0]
    for s in range(1, sources):
        highest = jnp.maximum(highest, stats[s][0])
    keeps = [jnp.exp2(jnp.where(lane < heads, m - highest, 0.0)) for m, _ in stats]
    total = keeps[0] * stats[0][1]
    for s in range(1, sources):
        total = total + keeps[s] * stats[s][1]
    for head in range(heads):
        cut = slice(head * HD, (head + 1) * HD)
        summed = in_ref[0, :, cut].astype(F32) * keeps[0][:, head : head + 1]
        for s in range(1, sources):
            summed = summed + in_ref[s, :, cut].astype(F32) * keeps[s][:, head : head + 1]
        out_ref[:, cut] = summed.astype(BF16)
    out_ref[:, at:] = split_stats(lane, highest, total, heads).astype(BF16)


def fold(received):
    sources, rows, width = received.shape
    return pl.pallas_call(
        fold_body,
        out_shape=jax.ShapeDtypeStruct((rows, width), BF16),
        name="fold",
    )(received)


def finish_body(in_ref, out_ref, *, group):
    rows, width = in_ref.shape
    heads = (width - HD) // HD
    at = heads * HD
    lane = lax.broadcasted_iota(jnp.int32, (rows, HD), 1)
    peak, total = joined_stats(in_ref[:, at:].astype(F32), heads)
    peak = jnp.where(lane < heads, peak, 0.0)
    highest = peak
    shift = group
    while shift < rows:
        highest = jnp.maximum(highest, pltpu.roll(highest, shift, 0))
        shift *= 2
    keep = jnp.exp2(peak - highest)
    total = keep * total

    def over_sources(x):
        size = 8
        y = x[:size]
        for first in range(size, rows, size):
            y = y + x[first : first + size]
        shift = group
        while shift < size:
            y = y + pltpu.roll(y, shift, 0)
            shift *= 2
        return y

    total = over_sources(total)
    for head in range(heads):
        cut = slice(head * HD, (head + 1) * HD)
        summed = over_sources(in_ref[:, cut].astype(F32) * keep[:, head : head + 1])
        out_ref[:, cut] = (summed / total[:, head : head + 1]).astype(BF16)


def finish(received):
    sources, group, width = received.shape
    flat = received.reshape(sources * group, width)
    out = pl.pallas_call(
        lambda *refs: finish_body(*refs, group=group),
        out_shape=jax.ShapeDtypeStruct((8, width - HD), BF16),
        name="finish",
    )(flat)
    return out[:group]


def close_body(att_ref, weight_ref, out_ref):
    pieces, rows, depth = att_ref.shape
    total = dot_f32(att_ref[0], weight_ref[:depth, :])
    for c in range(1, pieces):
        total = total + dot_f32(att_ref[c], weight_ref[c * depth : (c + 1) * depth, :])
    halves = out_ref.shape[0]
    columns = out_ref.shape[2]
    for w in range(halves):
        out_ref[w] = total[:, w * columns : (w + 1) * columns]


def close(attention, out_weight, halves):
    pieces, rows, depth = attention.shape
    return pl.pallas_call(
        close_body,
        out_shape=jax.ShapeDtypeStruct((halves, rows, out_weight.shape[1] // halves), F32),
        name="close",
    )(attention, out_weight)


def span_projection(span_tokens, kv_weight, after):
    xs = lax.axis_size("x")
    tokens, half = span_tokens.shape
    x = lax.axis_index("x")
    weights = lax.all_gather(kv_weight, "z", axis=0, tiled=True)
    depth = weights.shape[0]
    per_core = half // depth
    order = [(a, w) for a in range(xs) for w in range(2)]

    def flat(a, w):
        return a * 2 + w

    first = [(flat(a, w), flat(2 * w + (a & 1), a >> 1)) for a, w in order]
    second = [(flat(a, w), flat(2 * w + 1 - (a & 1), a >> 1)) for a, w in order]
    low = span_tokens[:, :depth]
    high = span_tokens[:, depth:]
    odd = (x & 1) == 1
    one = lax.ppermute(jnp.where(odd, high, low), ("x", "width"), first)
    two = lax.ppermute(jnp.where(odd, low, high), ("x", "width"), second)
    mine = jnp.stack([jnp.where(odd, two, one), jnp.where(odd, one, two)])
    theirs = lax.ppermute(mine, "width", [(0, 1), (1, 0)])
    upper = lax.axis_index("width") == 1
    ready = jnp.concatenate(
        [jnp.where(upper, theirs, mine), jnp.where(upper, mine, theirs)], axis=0
    )
    ready, after = lax.optimization_barrier((ready, after))
    partial = dot_f32(ready.reshape(xs * tokens, depth), weights)
    partial = partial.reshape(xs, tokens, kv_weight.shape[1])
    return jnp.sum(exchanged(partial, "x"), axis=0).astype(BF16), after


def local(
    span_tokens,
    kv_weight,
    query_weight,
    out_weight,
    cache_keys,
    cache_values,
    hidden,
    lengths,
    offset,
):
    xs = lax.axis_size("x")
    zs = lax.axis_size("z")
    step_count, branch_count, depth = hidden.shape
    rows = step_count * branch_count
    states = hidden.reshape(rows, depth)
    slots = cache_keys.shape[0]
    span = span_tokens.shape[0]
    scale = LOG2E / math.sqrt(HD)

    partial = project(states, query_weight, kv_weight, xs)
    own = jnp.sum(exchanged(partial, "x"), axis=0)
    own = own.reshape(zs, rows // zs, own.shape[1])
    own = jnp.sum(exchanged(own, "z"), axis=0).astype(BF16)
    columns = copies_from(own, "z").reshape(rows, own.shape[1])
    projected = copies_from(columns, "x")

    span_kv, projected = span_projection(span_tokens, kv_weight, projected)

    seat = lax.axis_index(SEQ)
    visible = jnp.tile(jnp.minimum(lengths, offset[0]), step_count)[:, None]
    places = seat * slots + jnp.arange(slots, dtype=jnp.int32)[None]
    row = jnp.arange(rows, dtype=jnp.int32)
    same = (row[:, None] % branch_count == row[None] % branch_count) & (row[None] <= row[:, None])
    filler = -(slots + span + rows) % HD
    allowed = jnp.concatenate(
        [
            places < visible,
            jnp.ones((rows, span), jnp.bool_),
            same & (seat == 0),
            jnp.zeros((rows, filler), jnp.bool_),
        ],
        axis=1,
    )
    bias = jnp.where(allowed, 0.0, MASKED_SCORE).astype(F32)
    keys = cache_keys.transpose(1, 0, 2)
    values = cache_values.transpose(1, 0, 2)

    partial = attend(projected, keys, values, span_kv, bias, scale)
    folded = fold(exchanged(partial, "x"))
    folded = folded.reshape(zs, rows // zs, folded.shape[1])
    attention = finish(exchanged(folded, "z"))
    columns = copies_from(attention, "z").reshape(rows, attention.shape[1])
    whole = copies_from(columns, "x")
    halves = exchanged(close(whole, out_weight, 2), "width")
    attended = (halves[0] + halves[1]).astype(BF16)
    return (span_kv, attended.reshape(step_count, branch_count, attended.shape[1]))


def solution(mesh):
    finer = Mesh(
        mesh.devices.reshape(mesh.shape["groups"], 4, 16, mesh.shape["width"]),
        ("groups", "x", "z", "width"),
    )
    placed = (
        P(GROUPS_SEQ, "width"),
        P(SEQ, "width"),
        P(SEQ, "width"),
        P("width", SEQ),
        P(GROUPS_SEQ, "width", None),
        P(GROUPS_SEQ, "width", None),
        P(None, "groups", SEQ),
        P("groups"),
        P("groups"),
    )
    return jax.shard_map(
        local,
        mesh=finer,
        in_specs=placed,
        out_specs=(P(GROUPS_SEQ, "width"), P(None, "groups", SEQ_WIDTH)),
        check_vma=False,
    )
```

```python
import math

import jax
import jax.numpy as jnp
from jax import lax
from jax.experimental import pallas as pl
from jax.experimental.pallas import tpu as pltpu
from jax.sharding import Mesh
from jax.sharding import PartitionSpec as P


HD = 128
SEQ = ("x", "z")
GROUPS_SEQ = ("groups", "x", "z")
SEQ_WIDTH = ("x", "z", "width")
MASKED_SCORE = -1e30
LOG2E = 1.4426950408889634
F32 = jnp.float32
BF16 = jnp.bfloat16
TILE = 8


def exchanged(pieces, axis):
    return lax.all_to_all(pieces, axis, split_axis=0, concat_axis=0, tiled=True)


def dot_f32(a, b):
    return jnp.dot(a, b, preferred_element_type=F32)


def on_chip(body, outs, *operands, scratch=(), free=()):
    shapes = jax.tree.map(lambda o: pltpu.VMEM(o.shape, o.dtype), outs)
    placed = [
        x if i in free else pltpu.with_memory_space_constraint(x, pltpu.VMEM)
        for i, x in enumerate(operands)
    ]
    params = pltpu.CompilerParams(vmem_limit_bytes=16 * 2**20)
    return pl.pallas_call(
        body, out_shape=shapes, scratch_shapes=scratch, compiler_params=params
    )(*placed)


def array(shape, dtype):
    return jax.ShapeDtypeStruct(shape, dtype)


def parts_of(rows, places):
    return places // (rows // TILE)


def project(states, query_weight, kv_weight, pieces):
    rows, _ = states.shape
    columns = query_weight.shape[1] // pieces
    extra = kv_weight.shape[1] // pieces

    def body(states_hbm, query_hbm, fresh_hbm, out_ref, states_ref, query_ref, fresh_ref, sems):
        copies = [
            pltpu.make_async_copy(states_hbm, states_ref, sems.at[0]),
            pltpu.make_async_copy(fresh_hbm, fresh_ref, sems.at[1]),
        ]
        for c in range(pieces):
            cut = slice(c * columns, (c + 1) * columns)
            copies.append(
                pltpu.make_async_copy(query_hbm.at[:, cut], query_ref.at[:, cut], sems.at[2 + c])
            )
        for copy in copies:
            copy.start()
        copies[0].wait()
        copies[1].wait()
        states = states_ref[...]
        for c in range(pieces):
            copies[2 + c].wait()
            out_ref[c, :, :columns] = dot_f32(states, query_ref[:, c * columns : (c + 1) * columns])
            out_ref[c, :, columns:] = dot_f32(states, fresh_ref[:, c * extra : (c + 1) * extra])

    anywhere = pl.BlockSpec(memory_space=pltpu.HBM)
    return pl.pallas_call(
        body,
        in_specs=[anywhere, anywhere, anywhere],
        out_shape=pltpu.VMEM((pieces, rows, columns + extra), F32),
        scratch_shapes=[
            pltpu.VMEM(states.shape, BF16),
            pltpu.VMEM(query_weight.shape, BF16),
            pltpu.VMEM(kv_weight.shape, BF16),
            pltpu.SemaphoreType.DMA((2 + pieces,)),
        ],
        compiler_params=pltpu.CompilerParams(vmem_limit_bytes=16 * 2**20),
        name="project",
    )(*[pltpu.with_memory_space_constraint(x, pltpu.HBM) for x in (states, query_weight, kv_weight)])


def add_over_x(received, places):
    sources, rows, width = received.shape
    parts = parts_of(rows, places)
    columns = (width - HD) // parts

    def body(in_ref, out_ref):
        total = in_ref[0]
        for s in range(1, sources):
            total = total + in_ref[s]
        for part in range(parts):
            for group in range(rows // TILE):
                place = part * (rows // TILE) + group
                some = total[group * TILE : (group + 1) * TILE]
                out_ref[place, :, :columns] = some[:, part * columns : (part + 1) * columns]
                out_ref[place, :, columns:] = some[:, width - HD :]

    return on_chip(body, array((places, TILE, columns + HD), F32), received)


def add_over_z(received):
    def body(in_ref, out_ref):
        total = in_ref[0]
        for s in range(1, in_ref.shape[0]):
            total = total + in_ref[s]
        total = total.astype(BF16)
        for s in range(in_ref.shape[0]):
            out_ref[s] = total

    return on_chip(body, array(received.shape, BF16), received)


def fan(received, rows, copies, tail):
    places, _, width = received.shape
    parts = parts_of(rows, places)
    columns = width - tail
    whole = parts * columns + tail

    def body(in_ref, out_ref):
        for part in range(parts):
            for pair in range(rows // TILE // 2):
                place = part * (rows // TILE) + 2 * pair
                some = jnp.concatenate(
                    [in_ref[place].astype(F32), in_ref[place + 1].astype(F32)], axis=0
                ).astype(BF16)
                at = slice(2 * pair * TILE, 2 * (pair + 1) * TILE)
                for c in range(copies):
                    out_ref[c, at, part * columns : (part + 1) * columns] = some[:, :columns]
                    if tail and part == 0:
                        out_ref[c, at, parts * columns :] = some[:, columns:]

    return on_chip(body, array((copies, rows, whole), BF16), received)


def three_parts(x):
    high = x.astype(BF16).astype(F32)
    rest = x - high
    middle = rest.astype(BF16).astype(F32)
    return (high, middle, rest - middle)


def joined_stats(tail, heads):
    lanes = tail.shape[-1]
    whole = tail + pltpu.roll(tail, lanes - heads, 1) + pltpu.roll(tail, lanes - 2 * heads, 1)
    return whole, pltpu.roll(whole, lanes - 3 * heads, 1)


def split_stats(highest, total, heads):
    lane = lax.broadcasted_iota(jnp.int32, highest.shape, 1)
    parts = (*three_parts(highest), *three_parts(total))
    stats = jnp.where(lane < heads, parts[0], 0.0)
    for place in range(1, 6):
        here = (lane >= place * heads) & (lane < (place + 1) * heads)
        stats = jnp.where(here, pltpu.roll(parts[place], place * heads, 1), stats)
    return stats


def heads_together(ref, piece, first, count):
    return jnp.concatenate(
        [ref[piece, :, (first + i) * HD : (first + i + 1) * HD] for i in range(count)], axis=0
    )


def score(q, keys):
    return lax.dot_general(q, keys, (((1,), (1,)), ((), ())), preferred_element_type=F32)


def attend(projected, keys, values, bias, scale):
    pieces, rows, width = projected.shape
    local_heads, slots, _ = keys.shape
    per_head = pieces // local_heads
    total_keys = bias.shape[1]
    heads = (width - HD) // HD
    per_dot = 256 // rows
    at = heads * HD
    blank_rows = total_keys - slots - rows

    def body(q_ref, keys_ref, values_ref, bias_ref, out_ref, stats_ref, k_ref, v_ref):
        bias = bias_ref[...]
        lane = lax.broadcasted_iota(jnp.int32, (rows, HD), 1)
        blank = [jnp.zeros((blank_rows, HD), BF16)] if blank_rows else []
        for h in range(local_heads):
            k_ref[h, :slots, :] = keys_ref[h]
            v_ref[h, :slots, :] = values_ref[h]
            for place, into in ((h * per_head, k_ref), (h * per_head + 1, v_ref)):
                into[h, slots:, :] = jnp.concatenate(
                    [q_ref[place, :, at:]] + blank, axis=0
                )
        for h in range(local_heads):
            for piece in range(h * per_head, (h + 1) * per_head):
                peaks = jnp.zeros((rows, HD), F32)
                totals = jnp.zeros((rows, HD), F32)
                for first in range(0, heads, per_dot):
                    q = heads_together(q_ref, piece, first, per_dot)
                    scores = score(q, k_ref[h])
                    scores = scores.reshape(per_dot, rows, total_keys) * scale + bias[None]
                    highest = jnp.max(scores, axis=-1, keepdims=True)
                    weights = jnp.exp2(scores - highest)
                    total = jnp.sum(weights, axis=-1, keepdims=True)
                    weights = weights.reshape(per_dot * rows, total_keys).astype(BF16)
                    summed = dot_f32(weights, v_ref[h])
                    for i in range(per_dot):
                        head = first + i
                        out_ref[piece, :, head * HD : (head + 1) * HD] = summed[
                            i * rows : (i + 1) * rows
                        ]
                        peaks = jnp.where(lane == head, highest[i], peaks)
                        totals = jnp.where(lane == head, total[i], totals)
                stats_ref[piece, 0] = peaks
                stats_ref[piece, 1] = totals

    outs = [array((pieces, rows, at), F32), array((pieces, 2, rows, HD), F32)]
    scratch = [pltpu.VMEM((local_heads, total_keys, HD), BF16)] * 2
    return on_chip(body, outs, projected, keys, values, bias, scratch=scratch)


def with_span(projected, summed, stats, span_kv, scale):
    pieces, rows, width = projected.shape
    heads = (width - HD) // HD
    per_dot = 256 // rows
    at = heads * HD
    local_heads = span_kv.shape[1] // (2 * HD)
    per_head = pieces // local_heads

    def body(q_ref, summed_ref, stats_ref, span_ref, out_ref):
        lane = lax.broadcasted_iota(jnp.int32, (rows, HD), 1)
        for piece in range(pieces):
            begin = (piece // per_head) * 2 * HD
            keys = span_ref[:, begin : begin + HD]
            values = span_ref[:, begin + HD : begin + 2 * HD]
            peaks = stats_ref[piece, 0]
            totals = stats_ref[piece, 1]
            new_peaks = jnp.zeros((rows, HD), F32)
            added = jnp.zeros((rows, HD), F32)
            for first in range(0, heads, per_dot):
                q = heads_together(q_ref, piece, first, per_dot)
                scores = score(q, keys).reshape(per_dot, rows, keys.shape[0]) * scale
                highest = jnp.max(scores, axis=-1, keepdims=True)
                old = [peaks[:, first + i : first + i + 1] for i in range(per_dot)]
                highest = jnp.maximum(highest, jnp.stack(old))
                weights = jnp.exp2(scores - highest)
                total = jnp.sum(weights, axis=-1, keepdims=True)
                weights = weights.reshape(per_dot * rows, keys.shape[0]).astype(BF16)
                extra = dot_f32(weights, values)
                for i in range(per_dot):
                    head = first + i
                    cut = slice(head * HD, (head + 1) * HD)
                    keep = jnp.exp2(old[i] - highest[i])
                    out_ref[piece, :, cut] = (
                        summed_ref[piece, :, cut] * keep + extra[i * rows : (i + 1) * rows]
                    ).astype(BF16)
                    new_peaks = jnp.where(lane == head, highest[i], new_peaks)
                    added = jnp.where(lane == head, total[i], added)
            kept = jnp.exp2(jnp.where(lane < heads, peaks - new_peaks, 0.0))
            stats = split_stats(new_peaks, totals * kept + added, heads)
            out_ref[piece, :, at:] = stats.astype(BF16)

    out = array((pieces, rows, width), BF16)
    return on_chip(body, out, projected, summed, stats, span_kv, free=(1,))


def fold(received, places):
    sources, rows, width = received.shape
    heads = (width - HD) // HD
    at = heads * HD
    parts = parts_of(rows, places)
    some_heads = heads // parts
    groups = rows // TILE
    columns = some_heads * HD

    def body(in_ref, out_ref):
        lane = lax.broadcasted_iota(jnp.int32, (rows, HD), 1)
        stats = [joined_stats(in_ref[s, :, at:].astype(F32), heads) for s in range(sources)]
        highest = stats[0][0]
        for s in range(1, sources):
            highest = jnp.maximum(highest, stats[s][0])
        keeps = [jnp.exp2(jnp.where(lane < heads, m - highest, 0.0)) for m, _ in stats]
        total = keeps[0] * stats[0][1]
        for s in range(1, sources):
            total = total + keeps[s] * stats[s][1]

        def put(part, cut, block):
            for group in range(groups):
                out_ref[part * groups + group, :, cut] = block[
                    group * TILE : (group + 1) * TILE
                ].astype(BF16)

        for part in range(parts):
            for i in range(some_heads):
                head = part * some_heads + i
                cut = slice(head * HD, (head + 1) * HD)
                summed = in_ref[0, :, cut].astype(F32) * keeps[0][:, head : head + 1]
                for s in range(1, sources):
                    keep = keeps[s][:, head : head + 1]
                    summed = summed + in_ref[s, :, cut].astype(F32) * keep
                put(part, slice(i * HD, (i + 1) * HD), summed)
            turn = (HD - part * some_heads) % HD
            peaks = pltpu.roll(highest, turn, 1) if turn else highest
            totals = pltpu.roll(total, turn, 1) if turn else total
            put(part, slice(columns, columns + HD), split_stats(peaks, totals, some_heads))

    return on_chip(body, array((places, TILE, columns + HD), BF16), received)


def finish(received):
    sources, group, width = received.shape
    heads = (width - HD) // HD
    at = heads * HD

    def body(in_ref, out_ref):
        lane = lax.broadcasted_iota(jnp.int32, (group, HD), 1)
        stats = [joined_stats(in_ref[s, :, at:].astype(F32), heads) for s in range(sources)]
        highest = stats[0][0]
        for s in range(1, sources):
            highest = jnp.maximum(highest, stats[s][0])
        keeps = [jnp.exp2(jnp.where(lane < heads, m - highest, 0.0)) for m, _ in stats]
        total = keeps[0] * stats[0][1]
        for s in range(1, sources):
            total = total + keeps[s] * stats[s][1]
        for head in range(heads):
            cut = slice(head * HD, (head + 1) * HD)
            summed = in_ref[0, :, cut].astype(F32) * keeps[0][:, head : head + 1]
            for s in range(1, sources):
                summed = summed + in_ref[s, :, cut].astype(F32) * keeps[s][:, head : head + 1]
            ready = (summed / total[:, head : head + 1]).astype(BF16)
            for s in range(sources):
                out_ref[s, :, cut] = ready

    return on_chip(body, array((sources, group, at), BF16), received)


def close(attention, out_weight, halves):
    pieces, rows, depth = attention.shape
    columns = out_weight.shape[1] // halves

    def body(in_ref, weight_ref, out_ref):
        total = dot_f32(in_ref[0], weight_ref[:depth, :])
        for c in range(1, pieces):
            total = total + dot_f32(in_ref[c], weight_ref[c * depth : (c + 1) * depth, :])
        for w in range(halves):
            out_ref[w] = total[:, w * columns : (w + 1) * columns]

    return on_chip(body, array((halves, rows, columns), F32), attention, out_weight)


def tokens_by_x(span_tokens, depth):
    xs = lax.axis_size("x")
    x = lax.axis_index("x")
    order = [(a, w) for a in range(xs) for w in range(2)]

    def flat(a, w):
        return a * 2 + w

    first = [(flat(a, w), flat(2 * w + (a & 1), a >> 1)) for a, w in order]
    second = [(flat(a, w), flat(2 * w + 1 - (a & 1), a >> 1)) for a, w in order]
    low = span_tokens[:, :depth]
    high = span_tokens[:, depth:]
    odd = (x & 1) == 1
    one = lax.ppermute(jnp.where(odd, high, low), ("x", "width"), first)
    two = lax.ppermute(jnp.where(odd, low, high), ("x", "width"), second)
    mine = jnp.stack([jnp.where(odd, two, one), jnp.where(odd, one, two)])
    theirs = lax.ppermute(mine, "width", [(0, 1), (1, 0)])
    upper = lax.axis_index("width") == 1
    return jnp.concatenate(
        [jnp.where(upper, theirs, mine), jnp.where(upper, mine, theirs)], axis=0
    )


def biases(lengths, offset, step_count, slots):
    branch_count = lengths.shape[0]
    rows = step_count * branch_count
    seat = lax.axis_index(SEQ)
    visible = jnp.tile(jnp.minimum(lengths, offset[0]), step_count)[:, None]
    places = seat * slots + jnp.arange(slots, dtype=jnp.int32)[None]
    row = jnp.arange(rows, dtype=jnp.int32)
    same = (row[:, None] % branch_count == row[None] % branch_count) & (row[None] <= row[:, None])
    filler = jnp.zeros((rows, -(slots + rows) % HD), jnp.bool_)
    allowed = jnp.concatenate([places < visible, same & (seat == 0), filler], axis=1)
    return jnp.where(allowed, 0.0, MASKED_SCORE).astype(F32)


def local(
    span_tokens,
    kv_weight,
    query_weight,
    out_weight,
    cache_keys,
    cache_values,
    hidden,
    lengths,
    offset,
):
    xs = lax.axis_size("x")
    zs = lax.axis_size("z")
    step_count, branch_count, depth = hidden.shape
    rows = step_count * branch_count
    scale = LOG2E / math.sqrt(HD)
    span_weight = lax.all_gather(kv_weight, "z", axis=0, tiled=True)
    tokens = span_tokens.shape[0]

    partial = project(hidden.reshape(rows, depth), query_weight, kv_weight, xs)
    partial = exchanged(partial, "x")
    partial, span_tokens = lax.optimization_barrier((partial, span_tokens))
    ready = tokens_by_x(span_tokens, span_weight.shape[0])
    partial = add_over_x(partial, zs)
    partial = exchanged(partial, "z")
    own = add_over_z(partial)
    own = exchanged(own, "z")
    columns = fan(own, rows, xs, HD)
    columns, ready = lax.optimization_barrier((columns, ready))
    projected = exchanged(columns, "x")

    span_partial = dot_f32(ready.reshape(xs * tokens, span_weight.shape[0]), span_weight)
    span_partial = span_partial.reshape(xs, tokens, kv_weight.shape[1])
    span_kv = jnp.sum(exchanged(span_partial, "x"), axis=0).astype(BF16)

    bias = biases(lengths, offset, step_count, cache_keys.shape[0])
    keys = cache_keys.transpose(1, 0, 2)
    values = cache_values.transpose(1, 0, 2)
    summed, stats = attend(projected, keys, values, bias, scale)
    partial = with_span(projected, summed, stats, span_kv, scale)
    folded = fold(exchanged(partial, "x"), zs)
    ours = finish(exchanged(folded, "z"))
    attention = exchanged(fan(exchanged(ours, "z"), rows, xs, 0), "x")
    halves = exchanged(close(attention, out_weight, 2), "width")
    attended = (halves[0] + halves[1]).astype(BF16)
    return (span_kv, attended.reshape(step_count, branch_count, attended.shape[1]))


def solution(mesh):
    finer = Mesh(
        mesh.devices.reshape(mesh.shape["groups"], 4, 16, mesh.shape["width"]),
        ("groups", "x", "z", "width"),
    )
    placed = (
        P(GROUPS_SEQ, "width"),
        P(SEQ, "width"),
        P(SEQ, "width"),
        P("width", SEQ),
        P(GROUPS_SEQ, "width", None),
        P(GROUPS_SEQ, "width", None),
        P(None, "groups", SEQ),
        P("groups"),
        P("groups"),
    )

    return jax.shard_map(
        local,
        mesh=finer,
        in_specs=placed,
        out_specs=(P(GROUPS_SEQ, "width"), P(None, "groups", SEQ_WIDTH)),
        check_vma=False,
    )
```

```python
import math

import jax
import jax.numpy as jnp
from jax import lax
from jax.experimental import pallas as pl
from jax.experimental.pallas import tpu as pltpu
from jax.sharding import Mesh
from jax.sharding import PartitionSpec as P


HD = 128
Z = ("zh", "zl")
SEQ = ("x", *Z)
GROUPS_SEQ = ("groups", *SEQ)
SEQ_WIDTH = (*SEQ, "width")
MASKED_SCORE = -1e30
LOG2E = 1.4426950408889634
F32 = jnp.float32
BF16 = jnp.bfloat16
TILE = 8


def exchanged(pieces, axis):
    return lax.all_to_all(pieces, axis, split_axis=0, concat_axis=0, tiled=True)


def dot_f32(a, b):
    return jnp.dot(a, b, preferred_element_type=F32)


def on_chip(body, outs, *operands, scratch=()):
    shapes = jax.tree.map(lambda o: pltpu.VMEM(o.shape, o.dtype), outs)
    placed = [pltpu.with_memory_space_constraint(x, pltpu.VMEM) for x in operands]
    params = pltpu.CompilerParams(vmem_limit_bytes=16 * 2**20)
    return pl.pallas_call(
        body, out_shape=shapes, scratch_shapes=scratch, compiler_params=params
    )(*placed)


def array(shape, dtype):
    return jax.ShapeDtypeStruct(shape, dtype)


def parts_of(rows, places):
    return places // (rows // TILE)


def project(states, query_weight, kv_weight, pieces):
    rows, _ = states.shape
    columns = query_weight.shape[1] // pieces
    extra = kv_weight.shape[1] // pieces

    def body(states_hbm, query_hbm, fresh_hbm, out_ref, states_ref, query_ref, fresh_ref, sems):
        copies = [
            pltpu.make_async_copy(states_hbm, states_ref, sems.at[0]),
            pltpu.make_async_copy(fresh_hbm, fresh_ref, sems.at[1]),
        ]
        for c in range(pieces):
            cut = slice(c * columns, (c + 1) * columns)
            copies.append(
                pltpu.make_async_copy(query_hbm.at[:, cut], query_ref.at[:, cut], sems.at[2 + c])
            )
        for copy in copies:
            copy.start()
        copies[0].wait()
        copies[1].wait()
        states = states_ref[...]
        for c in range(pieces):
            copies[2 + c].wait()
            out_ref[c, :, :columns] = dot_f32(states, query_ref[:, c * columns : (c + 1) * columns])
            out_ref[c, :, columns:] = dot_f32(states, fresh_ref[:, c * extra : (c + 1) * extra])

    anywhere = pl.BlockSpec(memory_space=pltpu.HBM)
    return pl.pallas_call(
        body,
        in_specs=[anywhere, anywhere, anywhere],
        out_shape=pltpu.VMEM((pieces, rows, columns + extra), F32),
        scratch_shapes=[
            pltpu.VMEM(states.shape, BF16),
            pltpu.VMEM(query_weight.shape, BF16),
            pltpu.VMEM(kv_weight.shape, BF16),
            pltpu.SemaphoreType.DMA((2 + pieces,)),
        ],
        compiler_params=pltpu.CompilerParams(vmem_limit_bytes=16 * 2**20),
        name="project",
    )(*[pltpu.with_memory_space_constraint(x, pltpu.HBM) for x in (states, query_weight, kv_weight)])


def add_over_x(received, places):
    sources, rows, width = received.shape
    parts = parts_of(rows, places)
    columns = (width - HD) // parts

    def body(in_ref, out_ref):
        total = in_ref[0]
        for s in range(1, sources):
            total = total + in_ref[s]
        for part in range(parts):
            for group in range(rows // TILE):
                place = part * (rows // TILE) + group
                some = total[group * TILE : (group + 1) * TILE]
                out_ref[place, :, :columns] = some[:, part * columns : (part + 1) * columns]
                out_ref[place, :, columns:] = some[:, width - HD :]

    return on_chip(body, array((places, TILE, columns + HD), F32), received)


def add_over_z(received):
    def body(in_ref, out_ref):
        total = in_ref[0]
        for s in range(1, in_ref.shape[0]):
            total = total + in_ref[s]
        total = total.astype(BF16)
        for s in range(in_ref.shape[0]):
            out_ref[s] = total

    return on_chip(body, array(received.shape, BF16), received)


def fan(received, rows, copies, tail):
    places, _, width = received.shape
    parts = parts_of(rows, places)
    columns = width - tail
    whole = parts * columns + tail

    def body(in_ref, out_ref):
        for part in range(parts):
            for pair in range(rows // TILE // 2):
                place = part * (rows // TILE) + 2 * pair
                some = jnp.concatenate(
                    [in_ref[place].astype(F32), in_ref[place + 1].astype(F32)], axis=0
                ).astype(BF16)
                at = slice(2 * pair * TILE, 2 * (pair + 1) * TILE)
                for c in range(copies):
                    out_ref[c, at, part * columns : (part + 1) * columns] = some[:, :columns]
                    if tail and part == 0:
                        out_ref[c, at, parts * columns :] = some[:, columns:]

    return on_chip(body, array((copies, rows, whole), BF16), received)


def three_parts(x):
    high = x.astype(BF16).astype(F32)
    rest = x - high
    middle = rest.astype(BF16).astype(F32)
    return (high, middle, rest - middle)


def joined_stats(tail, heads):
    lanes = tail.shape[-1]
    whole = tail + pltpu.roll(tail, lanes - heads, 1) + pltpu.roll(tail, lanes - 2 * heads, 1)
    return whole, pltpu.roll(whole, lanes - 3 * heads, 1)


def split_stats(highest, total, heads):
    lane = lax.broadcasted_iota(jnp.int32, highest.shape, 1)
    parts = (*three_parts(highest), *three_parts(total))
    stats = jnp.where(lane < heads, parts[0], 0.0)
    for place in range(1, 6):
        here = (lane >= place * heads) & (lane < (place + 1) * heads)
        stats = jnp.where(here, pltpu.roll(parts[place], place * heads, 1), stats)
    return stats


def heads_together(ref, piece, first, count):
    return jnp.concatenate(
        [ref[piece, :, (first + i) * HD : (first + i + 1) * HD] for i in range(count)], axis=0
    )


def score(q, keys):
    return lax.dot_general(q, keys, (((1,), (1,)), ((), ())), preferred_element_type=F32)


def attend(projected, keys, values, span_kv, bias, scale):
    pieces, rows, width = projected.shape
    local_heads, slots, _ = keys.shape
    span = span_kv.shape[0]
    per_head = pieces // local_heads
    total_keys = bias.shape[1]
    heads = (width - HD) // HD
    per_dot = 256 // rows
    at = heads * HD
    blank_rows = total_keys - slots - rows - span

    def body(q_ref, keys_ref, values_ref, span_ref, bias_ref, out_ref, k_ref, v_ref):
        bias = bias_ref[...]
        lane = lax.broadcasted_iota(jnp.int32, (rows, HD), 1)
        blank = [jnp.zeros((blank_rows, HD), BF16)] if blank_rows else []
        for h in range(local_heads):
            k_ref[h, :slots, :] = keys_ref[h]
            v_ref[h, :slots, :] = values_ref[h]
            for side, into in enumerate((k_ref, v_ref)):
                begin = (2 * h + side) * HD
                more = [span_ref[:, begin : begin + HD], q_ref[h * per_head + side, :, at:]]
                into[h, slots:, :] = jnp.concatenate(more + blank, axis=0)
        for h in range(local_heads):
            for piece in range(h * per_head, (h + 1) * per_head):
                peaks = jnp.zeros((rows, HD), F32)
                totals = jnp.zeros((rows, HD), F32)
                for first in range(0, heads, per_dot):
                    q = heads_together(q_ref, piece, first, per_dot)
                    scores = score(q, k_ref[h])
                    scores = scores.reshape(per_dot, rows, total_keys) * scale + bias[None]
                    highest = jnp.max(scores, axis=-1, keepdims=True)
                    weights = jnp.exp2(scores - highest)
                    total = jnp.sum(weights, axis=-1, keepdims=True)
                    weights = weights.reshape(per_dot * rows, total_keys).astype(BF16)
                    summed = dot_f32(weights, v_ref[h])
                    for i in range(per_dot):
                        head = first + i
                        out_ref[piece, :, head * HD : (head + 1) * HD] = summed[
                            i * rows : (i + 1) * rows
                        ].astype(BF16)
                        peaks = jnp.where(lane == head, highest[i], peaks)
                        totals = jnp.where(lane == head, total[i], totals)
                out_ref[piece, :, at:] = split_stats(peaks, totals, heads).astype(BF16)

    out = array((pieces, rows, width), BF16)
    scratch = [pltpu.VMEM((local_heads, total_keys, HD), BF16)] * 2
    return on_chip(body, out, projected, keys, values, span_kv, bias, scratch=scratch)


def fold(received, places):
    sources, rows, width = received.shape
    heads = (width - HD) // HD
    at = heads * HD
    parts = parts_of(rows, places)
    some_heads = heads // parts
    groups = rows // TILE
    columns = some_heads * HD

    def body(in_ref, out_ref):
        lane = lax.broadcasted_iota(jnp.int32, (rows, HD), 1)
        stats = [joined_stats(in_ref[s, :, at:].astype(F32), heads) for s in range(sources)]
        highest = stats[0][0]
        for s in range(1, sources):
            highest = jnp.maximum(highest, stats[s][0])
        keeps = [jnp.exp2(jnp.where(lane < heads, m - highest, 0.0)) for m, _ in stats]
        total = keeps[0] * stats[0][1]
        for s in range(1, sources):
            total = total + keeps[s] * stats[s][1]

        def put(part, cut, block):
            for group in range(groups):
                out_ref[part * groups + group, :, cut] = block[
                    group * TILE : (group + 1) * TILE
                ].astype(BF16)

        for part in range(parts):
            for i in range(some_heads):
                head = part * some_heads + i
                cut = slice(head * HD, (head + 1) * HD)
                summed = in_ref[0, :, cut].astype(F32) * keeps[0][:, head : head + 1]
                for s in range(1, sources):
                    keep = keeps[s][:, head : head + 1]
                    summed = summed + in_ref[s, :, cut].astype(F32) * keep
                put(part, slice(i * HD, (i + 1) * HD), summed)
            turn = (HD - part * some_heads) % HD
            peaks = pltpu.roll(highest, turn, 1) if turn else highest
            totals = pltpu.roll(total, turn, 1) if turn else total
            put(part, slice(columns, columns + HD), split_stats(peaks, totals, some_heads))

    return on_chip(body, array((places, TILE, columns + HD), BF16), received)


def finish(received):
    sources, group, width = received.shape
    heads = (width - HD) // HD
    at = heads * HD

    def body(in_ref, out_ref):
        lane = lax.broadcasted_iota(jnp.int32, (group, HD), 1)
        stats = [joined_stats(in_ref[s, :, at:].astype(F32), heads) for s in range(sources)]
        highest = stats[0][0]
        for s in range(1, sources):
            highest = jnp.maximum(highest, stats[s][0])
        keeps = [jnp.exp2(jnp.where(lane < heads, m - highest, 0.0)) for m, _ in stats]
        total = keeps[0] * stats[0][1]
        for s in range(1, sources):
            total = total + keeps[s] * stats[s][1]
        for head in range(heads):
            cut = slice(head * HD, (head + 1) * HD)
            summed = in_ref[0, :, cut].astype(F32) * keeps[0][:, head : head + 1]
            for s in range(1, sources):
                summed = summed + in_ref[s, :, cut].astype(F32) * keeps[s][:, head : head + 1]
            ready = (summed / total[:, head : head + 1]).astype(BF16)
            for s in range(sources):
                out_ref[s, :, cut] = ready

    return on_chip(body, array((sources, group, at), BF16), received)


def close(attention, out_weight, halves):
    pieces, rows, depth = attention.shape
    columns = out_weight.shape[1] // halves

    def body(in_ref, weight_ref, out_ref):
        total = dot_f32(in_ref[0], weight_ref[:depth, :])
        for c in range(1, pieces):
            total = total + dot_f32(in_ref[c], weight_ref[c * depth : (c + 1) * depth, :])
        for w in range(halves):
            out_ref[w] = total[:, w * columns : (w + 1) * columns]

    return on_chip(body, array((halves, rows, columns), F32), attention, out_weight)


def swapped_if(flag, x, axis):
    return jnp.where(flag, jnp.flip(x, axis), x)


def tokens_by_features(span_tokens, depth):
    xs, zh, zl = (lax.axis_size(a) for a in ("x", "zh", "zl"))
    tokens, _ = span_tokens.shape
    block = depth // zh
    x, side, core = (lax.axis_index(a) for a in ("x", "zl", "width"))
    pieces = span_tokens.reshape(tokens, 2, zh, zl, block).transpose(1, 3, 0, 2, 4)
    pieces = pieces.reshape(2, zl, tokens, depth)
    pieces = swapped_if((x & 1) == 1, pieces, 0)
    pieces = swapped_if(side == 1, pieces, 1)
    mine = []
    for i in range(2):
        for j in range(zl):
            pairs = []
            for a in range(xs):
                for b in range(zl):
                    for w in range(2):
                        to = ((2 * w + ((a & 1) ^ i)) * zl + (b ^ j)) * 2 + (a >> 1)
                        pairs.append(((a * zl + b) * 2 + w, to))
            mine.append(lax.ppermute(pieces[i, j], ("x", "zl", "width"), pairs))
    mine = jnp.stack(mine)
    theirs = lax.ppermute(mine, "width", [(0, 1), (1, 0)])
    ready = jnp.stack([mine, theirs])
    return swapped_if((core ^ (x >> 1)) == 1, ready, 0).reshape(-1, tokens, depth)


def added_at_home(partial):
    spots = lax.axis_size("x") * lax.axis_size("zl")
    total = partial[0]
    received = []
    for mask in range(1, spots):
        pairs = [(i, i ^ mask) for i in range(spots)]
        received.append(lax.ppermute(partial[mask], ("x", "zl"), pairs))
    for more in received:
        total = total + more
    return total.astype(BF16)


def biases(lengths, offset, step_count, slots, span):
    branch_count = lengths.shape[0]
    rows = step_count * branch_count
    seat = lax.axis_index(SEQ)
    visible = jnp.tile(jnp.minimum(lengths, offset[0]), step_count)[:, None]
    places = seat * slots + jnp.arange(slots, dtype=jnp.int32)[None]
    row = jnp.arange(rows, dtype=jnp.int32)
    same = (row[:, None] % branch_count == row[None] % branch_count) & (row[None] <= row[:, None])
    every = jnp.ones((rows, span), jnp.bool_)
    filler = jnp.zeros((rows, -(slots + span + rows) % HD), jnp.bool_)
    allowed = jnp.concatenate([places < visible, every, same & (seat == 0), filler], axis=1)
    return jnp.where(allowed, 0.0, MASKED_SCORE).astype(F32)


def local(
    span_tokens,
    kv_weight,
    query_weight,
    out_weight,
    cache_keys,
    cache_values,
    hidden,
    lengths,
    offset,
):
    xs = lax.axis_size("x")
    zs = lax.axis_size(Z)
    step_count, branch_count, depth = hidden.shape
    rows = step_count * branch_count
    scale = LOG2E / math.sqrt(HD)
    tokens = span_tokens.shape[0]
    span_weight = lax.all_gather(kv_weight, "zh", axis=0, tiled=True)

    partial = project(hidden.reshape(rows, depth), query_weight, kv_weight, xs)
    partial = exchanged(partial, "x")
    ready = tokens_by_features(span_tokens, span_weight.shape[0])
    partial = add_over_x(partial, zs)
    partial = exchanged(partial, Z)
    own = add_over_z(partial)
    own = exchanged(own, Z)
    span_partial = dot_f32(ready.reshape(-1, span_weight.shape[0]), span_weight)
    span_kv = added_at_home(span_partial.reshape(-1, tokens, kv_weight.shape[1]))
    columns = fan(own, rows, xs, HD)
    projected = exchanged(columns, "x")

    bias = biases(lengths, offset, step_count, cache_keys.shape[0], tokens)
    keys = cache_keys.transpose(1, 0, 2)
    values = cache_values.transpose(1, 0, 2)
    partial = attend(projected, keys, values, span_kv, bias, scale)
    folded = fold(exchanged(partial, "x"), zs)
    ours = finish(exchanged(folded, Z))
    attention = exchanged(fan(exchanged(ours, Z), rows, xs, 0), "x")
    halves = exchanged(close(attention, out_weight, 2), "width")
    attended = (halves[0] + halves[1]).astype(BF16)
    return (span_kv, attended.reshape(step_count, branch_count, attended.shape[1]))


def solution(mesh):
    finer = Mesh(
        mesh.devices.reshape(mesh.shape["groups"], 4, 8, 2, mesh.shape["width"]),
        ("groups", "x", "zh", "zl", "width"),
    )
    placed = (
        P(GROUPS_SEQ, "width"),
        P(SEQ, "width"),
        P(SEQ, "width"),
        P("width", SEQ),
        P(GROUPS_SEQ, "width", None),
        P(GROUPS_SEQ, "width", None),
        P(None, "groups", SEQ),
        P("groups"),
        P("groups"),
    )

    return jax.shard_map(
        local,
        mesh=finer,
        in_specs=placed,
        out_specs=(P(GROUPS_SEQ, "width"), P(None, "groups", SEQ_WIDTH)),
        check_vma=False,
    )
```

```python
import math

import jax
import jax.numpy as jnp
from jax import lax
from jax.experimental import pallas as pl
from jax.experimental.pallas import tpu as pltpu
from jax.sharding import Mesh
from jax.sharding import PartitionSpec as P


HD = 128
SEQ = ("x", "z")
GROUPS_SEQ = ("groups", *SEQ)
SEQ_WIDTH = (*SEQ, "width")
MASKED_SCORE = -1e30
LOG2E = 1.4426950408889634
F32 = jnp.float32
BF16 = jnp.bfloat16
TILE = 8


def exchanged(pieces, axis):
    return lax.all_to_all(pieces, axis, split_axis=0, concat_axis=0, tiled=True)


def dot_f32(a, b):
    return jnp.dot(a, b, preferred_element_type=F32)


def on_chip(body, outs, *operands, scratch=()):
    shapes = jax.tree.map(lambda o: pltpu.VMEM(o.shape, o.dtype), outs)
    placed = [pltpu.with_memory_space_constraint(x, pltpu.VMEM) for x in operands]
    params = pltpu.CompilerParams(vmem_limit_bytes=16 * 2**20)
    return pl.pallas_call(
        body, out_shape=shapes, scratch_shapes=scratch, compiler_params=params
    )(*placed)


def array(shape, dtype):
    return jax.ShapeDtypeStruct(shape, dtype)


def parts_of(rows, places):
    return places // (rows // TILE)


def project(states, query_weight, kv_weight, pieces):
    rows, _ = states.shape
    columns = query_weight.shape[1] // pieces
    extra = kv_weight.shape[1] // pieces

    def body(states_hbm, query_hbm, fresh_hbm, out_ref, states_ref, query_ref, fresh_ref, sems):
        copies = [
            pltpu.make_async_copy(states_hbm, states_ref, sems.at[0]),
            pltpu.make_async_copy(fresh_hbm, fresh_ref, sems.at[1]),
        ]
        for c in range(pieces):
            cut = slice(c * columns, (c + 1) * columns)
            copies.append(
                pltpu.make_async_copy(query_hbm.at[:, cut], query_ref.at[:, cut], sems.at[2 + c])
            )
        for copy in copies:
            copy.start()
        copies[0].wait()
        copies[1].wait()
        states = states_ref[...]
        for c in range(pieces):
            copies[2 + c].wait()
            out_ref[c, :, :columns] = dot_f32(states, query_ref[:, c * columns : (c + 1) * columns])
            out_ref[c, :, columns:] = dot_f32(states, fresh_ref[:, c * extra : (c + 1) * extra])

    anywhere = pl.BlockSpec(memory_space=pltpu.HBM)
    return pl.pallas_call(
        body,
        in_specs=[anywhere, anywhere, anywhere],
        out_shape=pltpu.VMEM((pieces, rows, columns + extra), F32),
        scratch_shapes=[
            pltpu.VMEM(states.shape, BF16),
            pltpu.VMEM(query_weight.shape, BF16),
            pltpu.VMEM(kv_weight.shape, BF16),
            pltpu.SemaphoreType.DMA((2 + pieces,)),
        ],
        compiler_params=pltpu.CompilerParams(vmem_limit_bytes=16 * 2**20),
        name="project",
    )(*[pltpu.with_memory_space_constraint(x, pltpu.HBM) for x in (states, query_weight, kv_weight)])


def add_over_x(received, places):
    sources, rows, width = received.shape
    parts = parts_of(rows, places)
    columns = (width - HD) // parts

    def body(in_ref, out_ref):
        total = in_ref[0]
        for s in range(1, sources):
            total = total + in_ref[s]
        for part in range(parts):
            for group in range(rows // TILE):
                place = part * (rows // TILE) + group
                some = total[group * TILE : (group + 1) * TILE]
                out_ref[place, :, :columns] = some[:, part * columns : (part + 1) * columns]
                out_ref[place, :, columns:] = some[:, width - HD :]

    return on_chip(body, array((places, TILE, columns + HD), F32), received)


def add_over_z(received):
    def body(in_ref, out_ref):
        total = in_ref[0]
        for s in range(1, in_ref.shape[0]):
            total = total + in_ref[s]
        total = total.astype(BF16)
        for s in range(in_ref.shape[0]):
            out_ref[s] = total

    return on_chip(body, array(received.shape, BF16), received)


def fan(received, rows, copies, tail):
    places, _, width = received.shape
    parts = parts_of(rows, places)
    columns = width - tail
    whole = parts * columns + tail

    def body(in_ref, out_ref):
        for part in range(parts):
            for pair in range(rows // TILE // 2):
                place = part * (rows // TILE) + 2 * pair
                some = jnp.concatenate(
                    [in_ref[place].astype(F32), in_ref[place + 1].astype(F32)], axis=0
                ).astype(BF16)
                at = slice(2 * pair * TILE, 2 * (pair + 1) * TILE)
                for c in range(copies):
                    out_ref[c, at, part * columns : (part + 1) * columns] = some[:, :columns]
                    if tail and part == 0:
                        out_ref[c, at, parts * columns :] = some[:, columns:]

    return on_chip(body, array((copies, rows, whole), BF16), received)


def three_parts(x):
    high = x.astype(BF16).astype(F32)
    rest = x - high
    middle = rest.astype(BF16).astype(F32)
    return (high, middle, rest - middle)


def joined_stats(tail, heads):
    lanes = tail.shape[-1]
    whole = tail + pltpu.roll(tail, lanes - heads, 1) + pltpu.roll(tail, lanes - 2 * heads, 1)
    return whole, pltpu.roll(whole, lanes - 3 * heads, 1)


def split_stats(highest, total, heads):
    lane = lax.broadcasted_iota(jnp.int32, highest.shape, 1)
    parts = (*three_parts(highest), *three_parts(total))
    stats = jnp.where(lane < heads, parts[0], 0.0)
    for place in range(1, 6):
        here = (lane >= place * heads) & (lane < (place + 1) * heads)
        stats = jnp.where(here, pltpu.roll(parts[place], place * heads, 1), stats)
    return stats


def heads_together(ref, piece, first, count):
    return jnp.concatenate(
        [ref[piece, :, (first + i) * HD : (first + i + 1) * HD] for i in range(count)], axis=0
    )


def score(q, keys):
    return lax.dot_general(q, keys, (((1,), (1,)), ((), ())), preferred_element_type=F32)


def attend(projected, keys, values, span_kv, bias, scale):
    pieces, rows, width = projected.shape
    local_heads, slots, _ = keys.shape
    span = span_kv.shape[0]
    per_head = pieces // local_heads
    total_keys = bias.shape[1]
    heads = (width - HD) // HD
    per_dot = 256 // rows
    at = heads * HD
    blank_rows = total_keys - slots - rows - span

    def body(q_ref, keys_ref, values_ref, span_ref, bias_ref, out_ref, k_ref, v_ref):
        bias = bias_ref[...]
        lane = lax.broadcasted_iota(jnp.int32, (rows, HD), 1)
        blank = [jnp.zeros((blank_rows, HD), BF16)] if blank_rows else []
        for h in range(local_heads):
            k_ref[h, :slots, :] = keys_ref[h]
            v_ref[h, :slots, :] = values_ref[h]
            for side, into in enumerate((k_ref, v_ref)):
                begin = (2 * h + side) * HD
                more = [span_ref[:, begin : begin + HD], q_ref[h * per_head + side, :, at:]]
                into[h, slots:, :] = jnp.concatenate(more + blank, axis=0)
        for h in range(local_heads):
            for piece in range(h * per_head, (h + 1) * per_head):
                peaks = jnp.zeros((rows, HD), F32)
                totals = jnp.zeros((rows, HD), F32)
                for first in range(0, heads, per_dot):
                    q = heads_together(q_ref, piece, first, per_dot)
                    scores = score(q, k_ref[h])
                    scores = scores.reshape(per_dot, rows, total_keys) * scale + bias[None]
                    highest = jnp.max(scores, axis=-1, keepdims=True)
                    weights = jnp.exp2(scores - highest)
                    total = jnp.sum(weights, axis=-1, keepdims=True)
                    weights = weights.reshape(per_dot * rows, total_keys).astype(BF16)
                    summed = dot_f32(weights, v_ref[h])
                    for i in range(per_dot):
                        head = first + i
                        out_ref[piece, :, head * HD : (head + 1) * HD] = summed[
                            i * rows : (i + 1) * rows
                        ].astype(BF16)
                        peaks = jnp.where(lane == head, highest[i], peaks)
                        totals = jnp.where(lane == head, total[i], totals)
                out_ref[piece, :, at:] = split_stats(peaks, totals, heads).astype(BF16)

    out = array((pieces, rows, width), BF16)
    scratch = [pltpu.VMEM((local_heads, total_keys, HD), BF16)] * 2
    return on_chip(body, out, projected, keys, values, span_kv, bias, scratch=scratch)


def fold(received, places):
    sources, rows, width = received.shape
    heads = (width - HD) // HD
    at = heads * HD
    parts = parts_of(rows, places)
    some_heads = heads // parts
    groups = rows // TILE
    columns = some_heads * HD

    def body(in_ref, out_ref):
        lane = lax.broadcasted_iota(jnp.int32, (rows, HD), 1)
        stats = [joined_stats(in_ref[s, :, at:].astype(F32), heads) for s in range(sources)]
        highest = stats[0][0]
        for s in range(1, sources):
            highest = jnp.maximum(highest, stats[s][0])
        keeps = [jnp.exp2(jnp.where(lane < heads, m - highest, 0.0)) for m, _ in stats]
        total = keeps[0] * stats[0][1]
        for s in range(1, sources):
            total = total + keeps[s] * stats[s][1]

        def put(part, cut, block):
            for group in range(groups):
                out_ref[part * groups + group, :, cut] = block[
                    group * TILE : (group + 1) * TILE
                ].astype(BF16)

        for part in range(parts):
            for i in range(some_heads):
                head = part * some_heads + i
                cut = slice(head * HD, (head + 1) * HD)
                summed = in_ref[0, :, cut].astype(F32) * keeps[0][:, head : head + 1]
                for s in range(1, sources):
                    keep = keeps[s][:, head : head + 1]
                    summed = summed + in_ref[s, :, cut].astype(F32) * keep
                put(part, slice(i * HD, (i + 1) * HD), summed)
            turn = (HD - part * some_heads) % HD
            peaks = pltpu.roll(highest, turn, 1) if turn else highest
            totals = pltpu.roll(total, turn, 1) if turn else total
            put(part, slice(columns, columns + HD), split_stats(peaks, totals, some_heads))

    return on_chip(body, array((places, TILE, columns + HD), BF16), received)


def finish(received):
    sources, group, width = received.shape
    heads = (width - HD) // HD
    at = heads * HD

    def body(in_ref, out_ref):
        lane = lax.broadcasted_iota(jnp.int32, (group, HD), 1)
        stats = [joined_stats(in_ref[s, :, at:].astype(F32), heads) for s in range(sources)]
        highest = stats[0][0]
        for s in range(1, sources):
            highest = jnp.maximum(highest, stats[s][0])
        keeps = [jnp.exp2(jnp.where(lane < heads, m - highest, 0.0)) for m, _ in stats]
        total = keeps[0] * stats[0][1]
        for s in range(1, sources):
            total = total + keeps[s] * stats[s][1]
        for head in range(heads):
            cut = slice(head * HD, (head + 1) * HD)
            summed = in_ref[0, :, cut].astype(F32) * keeps[0][:, head : head + 1]
            for s in range(1, sources):
                summed = summed + in_ref[s, :, cut].astype(F32) * keeps[s][:, head : head + 1]
            ready = (summed / total[:, head : head + 1]).astype(BF16)
            for s in range(sources):
                out_ref[s, :, cut] = ready

    return on_chip(body, array((sources, group, at), BF16), received)


def close(attention, out_weight, halves):
    pieces, rows, depth = attention.shape
    columns = out_weight.shape[1] // halves

    def body(in_ref, weight_ref, out_ref):
        total = dot_f32(in_ref[0], weight_ref[:depth, :])
        for c in range(1, pieces):
            total = total + dot_f32(in_ref[c], weight_ref[c * depth : (c + 1) * depth, :])
        for w in range(halves):
            out_ref[w] = total[:, w * columns : (w + 1) * columns]

    return on_chip(body, array((halves, rows, columns), F32), attention, out_weight)


def swapped_if(flag, x, axis):
    return jnp.where(flag, jnp.flip(x, axis), x)


def halves_of_blocks(span_tokens, places):
    tokens, width = span_tokens.shape
    block = width // (4 * places)

    def body(in_ref, out_ref):
        for k in range(2):
            for place in range(places):
                for half in range(2):
                    begin = ((k * places + place) * 2 + half) * block
                    cut = slice(place * block, (place + 1) * block)
                    out_ref[half, k, :, cut] = in_ref[:, begin : begin + block]

    out = array((2, 2, tokens, places * block), BF16)
    return on_chip(body, out, span_tokens)


def with_neighbour(x):
    count = lax.axis_size("groups")
    return lax.ppermute(x, "groups", [(g, g ^ 1) for g in range(count)])


def tokens_by_features(span_tokens, depth):
    xs, zs = (lax.axis_size(a) for a in ("x", "z"))
    tokens = span_tokens.shape[0]
    group, x, core = (lax.axis_index(a) for a in ("groups", "x", "width"))
    odd = (group & 1) == 1
    pieces = halves_of_blocks(span_tokens, zs)
    received = with_neighbour(jnp.where(odd, pieces[0], pieces[1]))
    both = jnp.stack([jnp.where(odd, pieces[1], pieces[0]), received], axis=1)
    both = swapped_if((x & 1) == 1, both, 0)
    mine = []
    for i in range(2):
        pairs = []
        for a in range(xs):
            for w in range(2):
                pairs.append((a * 2 + w, (2 * w + ((a & 1) ^ i)) * 2 + (a >> 1)))
        mine.append(lax.ppermute(both[i], ("x", "width"), pairs))
    mine = jnp.stack(mine)
    theirs = lax.ppermute(mine, "width", [(0, 1), (1, 0)])
    ready = jnp.stack([mine, theirs])
    return swapped_if((core ^ (x >> 1)) == 1, ready, 0).reshape(xs, 2, tokens, depth)


def added_at_home(partial):
    xs = lax.axis_size("x")
    received = with_neighbour(partial[:, 1])
    partial = partial[:, 0] + received
    total = partial[0]
    received = []
    for mask in range(1, xs):
        pairs = [(i, i ^ mask) for i in range(xs)]
        received.append(lax.ppermute(partial[mask], "x", pairs))
    for more in received:
        total = total + more
    return total.astype(BF16)


def biases(lengths, offset, step_count, slots, span):
    branch_count = lengths.shape[0]
    rows = step_count * branch_count
    seat = lax.axis_index(SEQ)
    visible = jnp.tile(jnp.minimum(lengths, offset[0]), step_count)[:, None]
    places = seat * slots + jnp.arange(slots, dtype=jnp.int32)[None]
    row = jnp.arange(rows, dtype=jnp.int32)
    same = (row[:, None] % branch_count == row[None] % branch_count) & (row[None] <= row[:, None])
    every = jnp.ones((rows, span), jnp.bool_)
    filler = jnp.zeros((rows, -(slots + span + rows) % HD), jnp.bool_)
    allowed = jnp.concatenate([places < visible, every, same & (seat == 0), filler], axis=1)
    return jnp.where(allowed, 0.0, MASKED_SCORE).astype(F32)


def local(
    span_tokens,
    kv_weight,
    query_weight,
    out_weight,
    cache_keys,
    cache_values,
    hidden,
    lengths,
    offset,
):
    xs = lax.axis_size("x")
    zs = lax.axis_size("z")
    step_count, branch_count, depth = hidden.shape
    rows = step_count * branch_count
    scale = LOG2E / math.sqrt(HD)
    tokens = span_tokens.shape[0]
    half = kv_weight.shape[0] // 2
    begin = (lax.axis_index("groups") & 1) * half
    span_weight = lax.dynamic_slice_in_dim(kv_weight, begin, half, 0)
    span_weight = lax.all_gather(span_weight, "z", axis=0, tiled=True)

    partial = project(hidden.reshape(rows, depth), query_weight, kv_weight, xs)
    partial = exchanged(partial, "x")
    ready = tokens_by_features(span_tokens, span_weight.shape[0])
    partial = add_over_x(partial, zs)
    partial = exchanged(partial, "z")
    own = add_over_z(partial)
    own = exchanged(own, "z")
    span_partial = dot_f32(ready.reshape(-1, span_weight.shape[0]), span_weight)
    span_kv = added_at_home(span_partial.reshape(xs, 2, tokens, kv_weight.shape[1]))
    columns = fan(own, rows, xs, HD)
    projected = exchanged(columns, "x")

    bias = biases(lengths, offset, step_count, cache_keys.shape[0], tokens)
    keys = cache_keys.transpose(1, 0, 2)
    values = cache_values.transpose(1, 0, 2)
    partial = attend(projected, keys, values, span_kv, bias, scale)
    folded = fold(exchanged(partial, "x"), zs)
    ours = finish(exchanged(folded, "z"))
    attention = exchanged(fan(exchanged(ours, "z"), rows, xs, 0), "x")
    halves = exchanged(close(attention, out_weight, 2), "width")
    attended = (halves[0] + halves[1]).astype(BF16)
    return (span_kv, attended.reshape(step_count, branch_count, attended.shape[1]))


def solution(mesh):
    finer = Mesh(
        mesh.devices.reshape(mesh.shape["groups"], 4, 16, mesh.shape["width"]),
        ("groups", "x", "z", "width"),
    )
    placed = (
        P(GROUPS_SEQ, "width"),
        P(SEQ, "width"),
        P(SEQ, "width"),
        P("width", SEQ),
        P(GROUPS_SEQ, "width", None),
        P(GROUPS_SEQ, "width", None),
        P(None, "groups", SEQ),
        P("groups"),
        P("groups"),
    )

    return jax.shard_map(
        local,
        mesh=finer,
        in_specs=placed,
        out_specs=(P(GROUPS_SEQ, "width"), P(None, "groups", SEQ_WIDTH)),
        check_vma=False,
    )
```

```python
import math

import jax
import jax.numpy as jnp
from jax import lax
from jax.experimental import pallas as pl
from jax.experimental.pallas import tpu as pltpu
from jax.sharding import Mesh
from jax.sharding import PartitionSpec as P


HD = 128
SEQ = ("x", "z")
GROUPS_SEQ = ("groups", *SEQ)
SEQ_WIDTH = (*SEQ, "width")
MASKED_SCORE = -1e30
LOG2E = 1.4426950408889634
F32 = jnp.float32
BF16 = jnp.bfloat16
TILE = 8


def exchanged(pieces, axis):
    return lax.all_to_all(pieces, axis, split_axis=0, concat_axis=0, tiled=True)


def dot_f32(a, b):
    return jnp.dot(a, b, preferred_element_type=F32)


def on_chip(body, outs, *operands, scratch=(), place=None):
    shapes = jax.tree.map(lambda o: pltpu.VMEM(o.shape, o.dtype), outs)
    placed = [pltpu.with_memory_space_constraint(x, pltpu.VMEM) for x in operands]
    specs = [pl.BlockSpec(memory_space=pltpu.VMEM)] * len(placed)
    if place is not None:
        placed.insert(0, place)
        specs.insert(0, pl.BlockSpec(memory_space=pltpu.SMEM))
    params = pltpu.CompilerParams(vmem_limit_bytes=16 * 2**20)
    return pl.pallas_call(
        body, in_specs=specs, out_shape=shapes, scratch_shapes=scratch, compiler_params=params
    )(*placed)


def exchanged_over_x(pieces):
    count = lax.axis_size("x")
    received = [pieces[0]]
    for mask in range(1, count):
        pairs = [(i, i ^ mask) for i in range(count)]
        received.append(lax.ppermute(pieces[mask], "x", pairs))
    return received


def array(shape, dtype):
    return jax.ShapeDtypeStruct(shape, dtype)


def parts_of(rows, places):
    return places // (rows // TILE)


def project(place, states, query_weight, kv_weight, pieces):
    rows, depth = states.shape
    columns = query_weight.shape[1] // pieces
    extra = kv_weight.shape[1] // pieces

    def body(place_ref, states_hbm, query_hbm, fresh_hbm, *rest):
        outs = rest[:pieces]
        states_ref, query_ref, fresh_ref, sems = rest[pieces:]
        x = place_ref[0]
        copies = [pltpu.make_async_copy(states_hbm, states_ref, sems.at[2 * pieces])]
        for m in range(pieces):
            c = x ^ m
            more = fresh_hbm.at[:, pl.ds(pl.multiple_of(c * extra, extra), extra)]
            most = query_hbm.at[:, pl.ds(pl.multiple_of(c * columns, columns), columns)]
            copies.append(pltpu.make_async_copy(more, fresh_ref.at[m], sems.at[2 * m]))
            copies.append(pltpu.make_async_copy(most, query_ref.at[m], sems.at[2 * m + 1]))
        for copy in copies:
            copy.start()
        copies[0].wait()
        states = states_ref[...]
        for m in range(pieces):
            copies[1 + 2 * m].wait()
            outs[m][:, columns:] = dot_f32(states, fresh_ref[m])
            copies[2 + 2 * m].wait()
            outs[m][:, :columns] = dot_f32(states, query_ref[m])

    hbm = [pltpu.with_memory_space_constraint(x, pltpu.HBM) for x in (states, query_weight, kv_weight)]
    return pl.pallas_call(
        body,
        in_specs=[pl.BlockSpec(memory_space=pltpu.SMEM)]
        + [pl.BlockSpec(memory_space=pltpu.HBM)] * len(hbm),
        out_shape=[pltpu.VMEM((rows, columns + extra), F32)] * pieces,
        scratch_shapes=[
            pltpu.VMEM(states.shape, BF16),
            pltpu.VMEM((pieces, depth, columns), BF16),
            pltpu.VMEM((pieces, depth, extra), BF16),
            pltpu.SemaphoreType.DMA((2 * pieces + 1,)),
        ],
        compiler_params=pltpu.CompilerParams(vmem_limit_bytes=16 * 2**20),
        name="project",
    )(place, *hbm)


def add_over_x(received, places):
    rows, width = received[0].shape
    parts = parts_of(rows, places)
    columns = (width - HD) // parts

    def body(*refs):
        out_ref = refs[-1]
        total = refs[0][...]
        for ref in refs[1:-1]:
            total = total + ref[...]
        for part in range(parts):
            for group in range(rows // TILE):
                place = part * (rows // TILE) + group
                some = total[group * TILE : (group + 1) * TILE]
                out_ref[place, :, :columns] = some[:, part * columns : (part + 1) * columns]
                out_ref[place, :, columns:] = some[:, width - HD :]

    return on_chip(body, array((places, TILE, columns + HD), F32), *received)


def add_over_z(received):
    def body(in_ref, out_ref):
        total = in_ref[0]
        for s in range(1, in_ref.shape[0]):
            total = total + in_ref[s]
        total = total.astype(BF16)
        for s in range(in_ref.shape[0]):
            out_ref[s] = total

    return on_chip(body, array(received.shape, BF16), received)


def fan(received, rows, tail):
    places, _, width = received.shape
    parts = parts_of(rows, places)
    columns = width - tail
    whole = parts * columns + tail

    def body(in_ref, out_ref):
        for part in range(parts):
            for pair in range(rows // TILE // 2):
                place = part * (rows // TILE) + 2 * pair
                some = jnp.concatenate(
                    [in_ref[place].astype(F32), in_ref[place + 1].astype(F32)], axis=0
                ).astype(BF16)
                at = slice(2 * pair * TILE, 2 * (pair + 1) * TILE)
                out_ref[at, part * columns : (part + 1) * columns] = some[:, :columns]
                if tail and part == 0:
                    out_ref[at, parts * columns :] = some[:, columns:]

    return on_chip(body, array((rows, whole), BF16), received)


def three_parts(x):
    high = x.astype(BF16).astype(F32)
    rest = x - high
    middle = rest.astype(BF16).astype(F32)
    return (high, middle, rest - middle)


def joined_stats(tail, heads):
    lanes = tail.shape[-1]
    whole = tail + pltpu.roll(tail, lanes - heads, 1) + pltpu.roll(tail, lanes - 2 * heads, 1)
    return whole, pltpu.roll(whole, lanes - 3 * heads, 1)


def split_stats(highest, total, heads):
    lane = lax.broadcasted_iota(jnp.int32, highest.shape, 1)
    parts = (*three_parts(highest), *three_parts(total))
    stats = jnp.where(lane < heads, parts[0], 0.0)
    for place in range(1, 6):
        here = (lane >= place * heads) & (lane < (place + 1) * heads)
        stats = jnp.where(here, pltpu.roll(parts[place], place * heads, 1), stats)
    return stats


def heads_together(ref, first, count):
    return jnp.concatenate(
        [ref[:, (first + i) * HD : (first + i + 1) * HD] for i in range(count)], axis=0
    )


def score(q, keys):
    return lax.dot_general(q, keys, (((1,), (1,)), ((), ())), preferred_element_type=F32)


def attend(place, projected, keys, values, span_kv, bias, scale):
    pieces = len(projected)
    rows, width = projected[0].shape
    local_heads, slots, _ = keys.shape
    span = span_kv.shape[0]
    per_head = pieces // local_heads
    total_keys = bias.shape[1]
    heads = (width - HD) // HD
    per_dot = 256 // rows
    at = heads * HD
    blank_rows = total_keys - slots - rows - span

    def body(place_ref, *refs):
        q_refs = refs[:pieces]
        keys_ref, values_ref, span_ref, bias_ref = refs[pieces : pieces + 4]
        outs = refs[pieces + 4 : 2 * pieces + 4]
        k_ref, v_ref = refs[2 * pieces + 4 :]
        x = place_ref[0]
        odd = (x & 1) == 1
        bias = bias_ref[...]
        lane = lax.broadcasted_iota(jnp.int32, (rows, HD), 1)
        blank = [jnp.zeros((blank_rows, HD), BF16)] if blank_rows else []
        for h in range(local_heads):
            head = (x >> 1) ^ h
            k_ref[h, :slots, :] = keys_ref[head]
            v_ref[h, :slots, :] = values_ref[head]
            first = q_refs[h * per_head][:, at:].astype(F32)
            second = q_refs[h * per_head + 1][:, at:].astype(F32)
            fresh = (jnp.where(odd, second, first), jnp.where(odd, first, second))
            for side, into in enumerate((k_ref, v_ref)):
                begin = pl.multiple_of((2 * head + side) * HD, HD)
                more = [span_ref[:, pl.ds(begin, HD)], fresh[side].astype(BF16)]
                into[h, slots:, :] = jnp.concatenate(more + blank, axis=0)
        for piece in range(pieces):
            h = piece // per_head
            peaks = jnp.zeros((rows, HD), F32)
            totals = jnp.zeros((rows, HD), F32)
            for first in range(0, heads, per_dot):
                q = heads_together(q_refs[piece], first, per_dot)
                scores = score(q, k_ref[h])
                scores = scores.reshape(per_dot, rows, total_keys) * scale + bias[None]
                highest = jnp.max(scores, axis=-1, keepdims=True)
                weights = jnp.exp2(scores - highest)
                total = jnp.sum(weights, axis=-1, keepdims=True)
                weights = weights.reshape(per_dot * rows, total_keys).astype(BF16)
                summed = dot_f32(weights, v_ref[h])
                for i in range(per_dot):
                    head = first + i
                    outs[piece][:, head * HD : (head + 1) * HD] = summed[
                        i * rows : (i + 1) * rows
                    ].astype(BF16)
                    peaks = jnp.where(lane == head, highest[i], peaks)
                    totals = jnp.where(lane == head, total[i], totals)
            outs[piece][:, at:] = split_stats(peaks, totals, heads).astype(BF16)

    out = [array((rows, width), BF16)] * pieces
    scratch = [pltpu.VMEM((local_heads, total_keys, HD), BF16)] * 2
    operands = (*projected, keys, values, span_kv, bias)
    return on_chip(body, out, *operands, scratch=scratch, place=place)


def fold(received, places):
    sources = len(received)
    rows, width = received[0].shape
    heads = (width - HD) // HD
    at = heads * HD
    parts = parts_of(rows, places)
    some_heads = heads // parts
    groups = rows // TILE
    columns = some_heads * HD

    def body(*refs):
        out_ref = refs[-1]
        lane = lax.broadcasted_iota(jnp.int32, (rows, HD), 1)
        stats = [joined_stats(refs[s][:, at:].astype(F32), heads) for s in range(sources)]
        highest = stats[0][0]
        for s in range(1, sources):
            highest = jnp.maximum(highest, stats[s][0])
        keeps = [jnp.exp2(jnp.where(lane < heads, m - highest, 0.0)) for m, _ in stats]
        total = keeps[0] * stats[0][1]
        for s in range(1, sources):
            total = total + keeps[s] * stats[s][1]

        def put(part, cut, block):
            for group in range(groups):
                out_ref[part * groups + group, :, cut] = block[
                    group * TILE : (group + 1) * TILE
                ].astype(BF16)

        for part in range(parts):
            for i in range(some_heads):
                head = part * some_heads + i
                cut = slice(head * HD, (head + 1) * HD)
                summed = refs[0][:, cut].astype(F32) * keeps[0][:, head : head + 1]
                for s in range(1, sources):
                    keep = keeps[s][:, head : head + 1]
                    summed = summed + refs[s][:, cut].astype(F32) * keep
                put(part, slice(i * HD, (i + 1) * HD), summed)
            turn = (HD - part * some_heads) % HD
            peaks = pltpu.roll(highest, turn, 1) if turn else highest
            totals = pltpu.roll(total, turn, 1) if turn else total
            put(part, slice(columns, columns + HD), split_stats(peaks, totals, some_heads))

    return on_chip(body, array((places, TILE, columns + HD), BF16), *received)


def finish(received):
    sources, group, width = received.shape
    heads = (width - HD) // HD
    at = heads * HD

    def body(in_ref, out_ref):
        lane = lax.broadcasted_iota(jnp.int32, (group, HD), 1)
        stats = [joined_stats(in_ref[s, :, at:].astype(F32), heads) for s in range(sources)]
        highest = stats[0][0]
        for s in range(1, sources):
            highest = jnp.maximum(highest, stats[s][0])
        keeps = [jnp.exp2(jnp.where(lane < heads, m - highest, 0.0)) for m, _ in stats]
        total = keeps[0] * stats[0][1]
        for s in range(1, sources):
            total = total + keeps[s] * stats[s][1]
        for head in range(heads):
            cut = slice(head * HD, (head + 1) * HD)
            summed = in_ref[0, :, cut].astype(F32) * keeps[0][:, head : head + 1]
            for s in range(1, sources):
                summed = summed + in_ref[s, :, cut].astype(F32) * keeps[s][:, head : head + 1]
            ready = (summed / total[:, head : head + 1]).astype(BF16)
            for s in range(sources):
                out_ref[s, :, cut] = ready

    return on_chip(body, array((sources, group, at), BF16), received)


def close(place, attention, out_weight):
    pieces = len(attention)
    rows, depth = attention[0].shape
    columns = out_weight.shape[1] // 2

    def body(place_ref, *refs):
        weight_ref, keep_ref, send_ref = refs[pieces:]
        total = None
        for m in range(pieces):
            begin = pl.multiple_of((place_ref[0] ^ m) * depth, depth)
            more = dot_f32(refs[m][...], weight_ref[pl.ds(begin, depth), :])
            total = more if total is None else total + more
        upper = place_ref[1] == 1
        left, right = total[:, :columns], total[:, columns:]
        keep_ref[...] = jnp.where(upper, right, left)
        send_ref[...] = jnp.where(upper, left, right)

    outs = [array((rows, columns), F32)] * 2
    return on_chip(body, outs, *attention, out_weight, place=place)


def swapped_if(flag, x, axis):
    return jnp.where(flag, jnp.flip(x, axis), x)


def halves_of_blocks(span_tokens, places):
    tokens, width = span_tokens.shape
    block = width // (4 * places)

    def body(in_ref, out_ref):
        for k in range(2):
            for place in range(places):
                for half in range(2):
                    begin = ((k * places + place) * 2 + half) * block
                    cut = slice(place * block, (place + 1) * block)
                    out_ref[half, k, :, cut] = in_ref[:, begin : begin + block]

    out = array((2, 2, tokens, places * block), BF16)
    return on_chip(body, out, span_tokens)


def with_neighbour(x):
    count = lax.axis_size("groups")
    return lax.ppermute(x, "groups", [(g, g ^ 1) for g in range(count)])


def tokens_by_features(span_tokens, depth):
    xs, zs = (lax.axis_size(a) for a in ("x", "z"))
    tokens = span_tokens.shape[0]
    group, x, core = (lax.axis_index(a) for a in ("groups", "x", "width"))
    odd = (group & 1) == 1
    pieces = halves_of_blocks(span_tokens, zs)
    received = with_neighbour(jnp.where(odd, pieces[0], pieces[1]))
    both = jnp.stack([jnp.where(odd, pieces[1], pieces[0]), received], axis=1)
    both = swapped_if((x & 1) == 1, both, 0)
    mine = []
    for i in range(2):
        pairs = []
        for a in range(xs):
            for w in range(2):
                pairs.append((a * 2 + w, (2 * w + ((a & 1) ^ i)) * 2 + (a >> 1)))
        mine.append(lax.ppermute(both[i], ("x", "width"), pairs))
    mine = jnp.stack(mine)
    theirs = lax.ppermute(mine, "width", [(0, 1), (1, 0)])
    ready = jnp.stack([mine, theirs])
    return swapped_if((core ^ (x >> 1)) == 1, ready, 0).reshape(xs, 2, tokens, depth)


def added_at_home(partial):
    xs = lax.axis_size("x")
    received = with_neighbour(partial[:, 1])
    partial = partial[:, 0] + received
    total = partial[0]
    received = []
    for mask in range(1, xs):
        pairs = [(i, i ^ mask) for i in range(xs)]
        received.append(lax.ppermute(partial[mask], "x", pairs))
    for more in received:
        total = total + more
    return total.astype(BF16)


def biases(lengths, offset, step_count, slots, span):
    branch_count = lengths.shape[0]
    rows = step_count * branch_count
    seat = lax.axis_index(SEQ)
    visible = jnp.tile(jnp.minimum(lengths, offset[0]), step_count)[:, None]
    places = seat * slots + jnp.arange(slots, dtype=jnp.int32)[None]
    row = jnp.arange(rows, dtype=jnp.int32)
    same = (row[:, None] % branch_count == row[None] % branch_count) & (row[None] <= row[:, None])
    every = jnp.ones((rows, span), jnp.bool_)
    filler = jnp.zeros((rows, -(slots + span + rows) % HD), jnp.bool_)
    allowed = jnp.concatenate([places < visible, every, same & (seat == 0), filler], axis=1)
    return jnp.where(allowed, 0.0, MASKED_SCORE).astype(F32)


def local(
    span_tokens,
    kv_weight,
    query_weight,
    out_weight,
    cache_keys,
    cache_values,
    hidden,
    lengths,
    offset,
):
    xs = lax.axis_size("x")
    zs = lax.axis_size("z")
    step_count, branch_count, depth = hidden.shape
    rows = step_count * branch_count
    scale = LOG2E / math.sqrt(HD)
    tokens = span_tokens.shape[0]
    half = kv_weight.shape[0] // 2
    begin = (lax.axis_index("groups") & 1) * half
    span_weight = lax.dynamic_slice_in_dim(kv_weight, begin, half, 0)
    span_weight = lax.all_gather(span_weight, "z", axis=0, tiled=True)

    place = jnp.stack([lax.axis_index("x"), lax.axis_index("width")])

    partial = project(place, hidden.reshape(rows, depth), query_weight, kv_weight, xs)
    partial = exchanged_over_x(partial)
    ready = tokens_by_features(span_tokens, span_weight.shape[0])
    partial = add_over_x(partial, zs)
    partial = exchanged(partial, "z")
    own = add_over_z(partial)
    own = exchanged(own, "z")
    span_partial = dot_f32(ready.reshape(-1, span_weight.shape[0]), span_weight)
    span_kv = added_at_home(span_partial.reshape(xs, 2, tokens, kv_weight.shape[1]))
    columns = fan(own, rows, HD)
    projected = exchanged_over_x([columns] * xs)

    bias = biases(lengths, offset, step_count, cache_keys.shape[0], tokens)
    keys = cache_keys.transpose(1, 0, 2)
    values = cache_values.transpose(1, 0, 2)
    partial = attend(place, projected, keys, values, span_kv, bias, scale)
    folded = fold(exchanged_over_x(partial), zs)
    ours = finish(exchanged(folded, "z"))
    columns = fan(exchanged(ours, "z"), rows, 0)
    attention = exchanged_over_x([columns] * xs)
    keep, send = close(place, attention, out_weight)
    attended = (keep + lax.ppermute(send, "width", [(0, 1), (1, 0)])).astype(BF16)
    return (span_kv, attended.reshape(step_count, branch_count, attended.shape[1]))


def solution(mesh):
    finer = Mesh(
        mesh.devices.reshape(mesh.shape["groups"], 4, 16, mesh.shape["width"]),
        ("groups", "x", "z", "width"),
    )
    placed = (
        P(GROUPS_SEQ, "width"),
        P(SEQ, "width"),
        P(SEQ, "width"),
        P("width", SEQ),
        P(GROUPS_SEQ, "width", None),
        P(GROUPS_SEQ, "width", None),
        P(None, "groups", SEQ),
        P("groups"),
        P("groups"),
    )

    return jax.shard_map(
        local,
        mesh=finer,
        in_specs=placed,
        out_specs=(P(GROUPS_SEQ, "width"), P(None, "groups", SEQ_WIDTH)),
        check_vma=False,
    )
```

```python
import math

import jax
import jax.numpy as jnp
from jax import lax
from jax.experimental import pallas as pl
from jax.experimental.pallas import tpu as pltpu
from jax.sharding import Mesh
from jax.sharding import PartitionSpec as P


HD = 128
SEQ = ("x", "z")
GROUPS_SEQ = ("groups", *SEQ)
SEQ_WIDTH = (*SEQ, "width")
MASKED_SCORE = -1e30
LOG2E = 1.4426950408889634
F32 = jnp.float32
BF16 = jnp.bfloat16
TILE = 8


def exchanged(pieces, axis):
    return lax.all_to_all(pieces, axis, split_axis=0, concat_axis=0, tiled=True)


def dot_f32(a, b):
    return jnp.dot(a, b, preferred_element_type=F32)


def on_chip(body, outs, *operands, scratch=(), place=None):
    shapes = jax.tree.map(lambda o: pltpu.VMEM(o.shape, o.dtype), outs)
    placed = [pltpu.with_memory_space_constraint(x, pltpu.VMEM) for x in operands]
    specs = [pl.BlockSpec(memory_space=pltpu.VMEM)] * len(placed)
    if place is not None:
        placed.insert(0, place)
        specs.insert(0, pl.BlockSpec(memory_space=pltpu.SMEM))
    params = pltpu.CompilerParams(vmem_limit_bytes=16 * 2**20)
    return pl.pallas_call(
        body, in_specs=specs, out_shape=shapes, scratch_shapes=scratch, compiler_params=params
    )(*placed)


def exchanged_over_x(pieces):
    count = lax.axis_size("x")
    received = [pieces[0]]
    for mask in range(1, count):
        pairs = [(i, i ^ mask) for i in range(count)]
        received.append(lax.ppermute(pieces[mask], "x", pairs))
    return received


def array(shape, dtype):
    return jax.ShapeDtypeStruct(shape, dtype)


def parts_of(rows, places):
    return places // (rows // TILE)


def project(place, states, query_weight, kv_weight, pieces):
    rows, depth = states.shape
    columns = query_weight.shape[1] // pieces
    extra = kv_weight.shape[1] // pieces

    def body(place_ref, states_hbm, query_hbm, fresh_hbm, *rest):
        outs = rest[:pieces]
        states_ref, query_ref, fresh_ref, sems = rest[pieces:]
        x = place_ref[0]
        copies = [pltpu.make_async_copy(states_hbm, states_ref, sems.at[2 * pieces])]
        for m in range(pieces):
            c = x ^ m
            more = fresh_hbm.at[:, pl.ds(pl.multiple_of(c * extra, extra), extra)]
            most = query_hbm.at[:, pl.ds(pl.multiple_of(c * columns, columns), columns)]
            copies.append(pltpu.make_async_copy(more, fresh_ref.at[m], sems.at[2 * m]))
            copies.append(pltpu.make_async_copy(most, query_ref.at[m], sems.at[2 * m + 1]))
        for copy in copies:
            copy.start()
        copies[0].wait()
        states = states_ref[...]
        for m in range(pieces):
            copies[1 + 2 * m].wait()
            outs[m][:, columns:] = dot_f32(states, fresh_ref[m])
            copies[2 + 2 * m].wait()
            outs[m][:, :columns] = dot_f32(states, query_ref[m])

    hbm = [pltpu.with_memory_space_constraint(x, pltpu.HBM) for x in (states, query_weight, kv_weight)]
    return pl.pallas_call(
        body,
        in_specs=[pl.BlockSpec(memory_space=pltpu.SMEM)]
        + [pl.BlockSpec(memory_space=pltpu.HBM)] * len(hbm),
        out_shape=[pltpu.VMEM((rows, columns + extra), F32)] * pieces,
        scratch_shapes=[
            pltpu.VMEM(states.shape, BF16),
            pltpu.VMEM((pieces, depth, columns), BF16),
            pltpu.VMEM((pieces, depth, extra), BF16),
            pltpu.SemaphoreType.DMA((2 * pieces + 1,)),
        ],
        compiler_params=pltpu.CompilerParams(vmem_limit_bytes=16 * 2**20),
        name="project",
    )(place, *hbm)


def add_over_x(received, places):
    rows, width = received[0].shape
    parts = parts_of(rows, places)
    columns = (width - HD) // parts

    def body(*refs):
        out_ref = refs[-1]
        total = refs[0][...]
        for ref in refs[1:-1]:
            total = total + ref[...]
        for part in range(parts):
            for group in range(rows // TILE):
                place = part * (rows // TILE) + group
                some = total[group * TILE : (group + 1) * TILE]
                out_ref[place, :, :columns] = some[:, part * columns : (part + 1) * columns]
                out_ref[place, :, columns:] = some[:, width - HD :]

    return on_chip(body, array((places, TILE, columns + HD), F32), *received)


def add_over_z(received):
    def body(in_ref, out_ref):
        total = in_ref[0]
        for s in range(1, in_ref.shape[0]):
            total = total + in_ref[s]
        total = total.astype(BF16)
        for s in range(in_ref.shape[0]):
            out_ref[s] = total

    return on_chip(body, array(received.shape, BF16), received)


def fan(received, rows, tail):
    places, _, width = received.shape
    parts = parts_of(rows, places)
    columns = width - tail
    whole = parts * columns + tail

    def body(in_ref, out_ref):
        for part in range(parts):
            for pair in range(rows // TILE // 2):
                place = part * (rows // TILE) + 2 * pair
                some = jnp.concatenate(
                    [in_ref[place].astype(F32), in_ref[place + 1].astype(F32)], axis=0
                ).astype(BF16)
                at = slice(2 * pair * TILE, 2 * (pair + 1) * TILE)
                out_ref[at, part * columns : (part + 1) * columns] = some[:, :columns]
                if tail and part == 0:
                    out_ref[at, parts * columns :] = some[:, columns:]

    return on_chip(body, array((rows, whole), BF16), received)


def three_parts(x):
    high = x.astype(BF16).astype(F32)
    rest = x - high
    middle = rest.astype(BF16).astype(F32)
    return (high, middle, rest - middle)


def joined_stats(tail, heads):
    lanes = tail.shape[-1]
    whole = tail + pltpu.roll(tail, lanes - heads, 1) + pltpu.roll(tail, lanes - 2 * heads, 1)
    return whole, pltpu.roll(whole, lanes - 3 * heads, 1)


def split_stats(highest, total, heads):
    lane = lax.broadcasted_iota(jnp.int32, highest.shape, 1)
    parts = (*three_parts(highest), *three_parts(total))
    stats = jnp.where(lane < heads, parts[0], 0.0)
    for place in range(1, 6):
        here = (lane >= place * heads) & (lane < (place + 1) * heads)
        stats = jnp.where(here, pltpu.roll(parts[place], place * heads, 1), stats)
    return stats


def heads_together(ref, first, count):
    return jnp.concatenate(
        [ref[:, (first + i) * HD : (first + i + 1) * HD] for i in range(count)], axis=0
    )


def score(q, keys):
    return lax.dot_general(q, keys, (((1,), (1,)), ((), ())), preferred_element_type=F32)


def attend(place, projected, keys, values, span_kv, bias, scale):
    pieces = len(projected)
    rows, width = projected[0].shape
    local_heads, slots, _ = keys.shape
    span = span_kv.shape[0]
    per_head = pieces // local_heads
    total_keys = bias.shape[1]
    heads = (width - HD) // HD
    per_dot = 256 // rows
    at = heads * HD
    blank_rows = total_keys - slots - rows - span

    def body(place_ref, *refs):
        q_refs = refs[:pieces]
        keys_ref, values_ref, span_ref, bias_ref = refs[pieces : pieces + 4]
        outs = refs[pieces + 4 : 2 * pieces + 4]
        k_ref, v_ref = refs[2 * pieces + 4 :]
        x = place_ref[0]
        odd = (x & 1) == 1
        bias = bias_ref[...]
        lane = lax.broadcasted_iota(jnp.int32, (rows, HD), 1)
        blank = [jnp.zeros((blank_rows, HD), BF16)] if blank_rows else []
        for h in range(local_heads):
            head = (x >> 1) ^ h
            k_ref[h, :slots, :] = keys_ref[head]
            v_ref[h, :slots, :] = values_ref[head]
            first = q_refs[h * per_head][:, at:].astype(F32)
            second = q_refs[h * per_head + 1][:, at:].astype(F32)
            fresh = (jnp.where(odd, second, first), jnp.where(odd, first, second))
            for side, into in enumerate((k_ref, v_ref)):
                begin = pl.multiple_of((2 * head + side) * HD, HD)
                more = [span_ref[:, pl.ds(begin, HD)], fresh[side].astype(BF16)]
                into[h, slots:, :] = jnp.concatenate(more + blank, axis=0)
        for piece in range(pieces):
            h = piece // per_head
            peaks = jnp.zeros((rows, HD), F32)
            totals = jnp.zeros((rows, HD), F32)
            for first in range(0, heads, per_dot):
                q = heads_together(q_refs[piece], first, per_dot)
                scores = score(q, k_ref[h])
                scores = scores.reshape(per_dot, rows, total_keys) * scale + bias[None]
                highest = jnp.max(scores, axis=-1, keepdims=True)
                weights = jnp.exp2(scores - highest)
                total = jnp.sum(weights, axis=-1, keepdims=True)
                weights = weights.reshape(per_dot * rows, total_keys).astype(BF16)
                summed = dot_f32(weights, v_ref[h])
                for i in range(per_dot):
                    head = first + i
                    outs[piece][:, head * HD : (head + 1) * HD] = summed[
                        i * rows : (i + 1) * rows
                    ].astype(BF16)
                    peaks = jnp.where(lane == head, highest[i], peaks)
                    totals = jnp.where(lane == head, total[i], totals)
            outs[piece][:, at:] = split_stats(peaks, totals, heads).astype(BF16)

    out = [array((rows, width), BF16)] * pieces
    scratch = [pltpu.VMEM((local_heads, total_keys, HD), BF16)] * 2
    operands = (*projected, keys, values, span_kv, bias)
    return on_chip(body, out, *operands, scratch=scratch, place=place)


def fold(received, places):
    sources = len(received)
    rows, width = received[0].shape
    heads = (width - HD) // HD
    at = heads * HD
    parts = parts_of(rows, places)
    some_heads = heads // parts
    groups = rows // TILE
    columns = some_heads * HD

    def body(*refs):
        out_ref = refs[-1]
        lane = lax.broadcasted_iota(jnp.int32, (rows, HD), 1)
        stats = [joined_stats(refs[s][:, at:].astype(F32), heads) for s in range(sources)]
        highest = stats[0][0]
        for s in range(1, sources):
            highest = jnp.maximum(highest, stats[s][0])
        keeps = [jnp.exp2(jnp.where(lane < heads, m - highest, 0.0)) for m, _ in stats]
        total = keeps[0] * stats[0][1]
        for s in range(1, sources):
            total = total + keeps[s] * stats[s][1]

        def put(part, cut, block):
            for group in range(groups):
                out_ref[part * groups + group, :, cut] = block[
                    group * TILE : (group + 1) * TILE
                ].astype(BF16)

        for part in range(parts):
            for i in range(some_heads):
                head = part * some_heads + i
                cut = slice(head * HD, (head + 1) * HD)
                summed = refs[0][:, cut].astype(F32) * keeps[0][:, head : head + 1]
                for s in range(1, sources):
                    keep = keeps[s][:, head : head + 1]
                    summed = summed + refs[s][:, cut].astype(F32) * keep
                put(part, slice(i * HD, (i + 1) * HD), summed)
            turn = (HD - part * some_heads) % HD
            peaks = pltpu.roll(highest, turn, 1) if turn else highest
            totals = pltpu.roll(total, turn, 1) if turn else total
            put(part, slice(columns, columns + HD), split_stats(peaks, totals, some_heads))

    return on_chip(body, array((places, TILE, columns + HD), BF16), *received)


def finish(received):
    sources, group, width = received.shape
    heads = (width - HD) // HD
    at = heads * HD

    def body(in_ref, out_ref):
        lane = lax.broadcasted_iota(jnp.int32, (group, HD), 1)
        stats = [joined_stats(in_ref[s, :, at:].astype(F32), heads) for s in range(sources)]
        highest = stats[0][0]
        for s in range(1, sources):
            highest = jnp.maximum(highest, stats[s][0])
        keeps = [jnp.exp2(jnp.where(lane < heads, m - highest, 0.0)) for m, _ in stats]
        total = keeps[0] * stats[0][1]
        for s in range(1, sources):
            total = total + keeps[s] * stats[s][1]
        for head in range(heads):
            cut = slice(head * HD, (head + 1) * HD)
            summed = in_ref[0, :, cut].astype(F32) * keeps[0][:, head : head + 1]
            for s in range(1, sources):
                summed = summed + in_ref[s, :, cut].astype(F32) * keeps[s][:, head : head + 1]
            ready = (summed / total[:, head : head + 1]).astype(BF16)
            for s in range(sources):
                out_ref[s, :, cut] = ready

    return on_chip(body, array((sources, group, at), BF16), received)


def close(place, attention, out_weight):
    pieces = len(attention)
    rows, depth = attention[0].shape
    columns = out_weight.shape[1] // 2

    def body(place_ref, *refs):
        weight_ref, keep_ref, send_ref = refs[pieces:]
        total = None
        for m in range(pieces):
            begin = pl.multiple_of((place_ref[0] ^ m) * depth, depth)
            more = dot_f32(refs[m][...], weight_ref[pl.ds(begin, depth), :])
            total = more if total is None else total + more
        upper = place_ref[1] == 1
        left, right = total[:, :columns], total[:, columns:]
        keep_ref[...] = jnp.where(upper, right, left)
        send_ref[...] = jnp.where(upper, left, right)

    outs = [array((rows, columns), F32)] * 2
    return on_chip(body, outs, *attention, out_weight, place=place)


def swapped_if(flag, x, axis):
    return jnp.where(flag, jnp.flip(x, axis), x)


def halves_of_blocks(span_tokens, places):
    tokens, width = span_tokens.shape
    block = width // (4 * places)

    def body(in_ref, out_ref):
        for k in range(2):
            for place in range(places):
                for half in range(2):
                    begin = ((k * places + place) * 2 + half) * block
                    cut = slice(place * block, (place + 1) * block)
                    out_ref[half, k, :, cut] = in_ref[:, begin : begin + block]

    out = array((2, 2, tokens, places * block), BF16)
    return on_chip(body, out, span_tokens)


def with_neighbour(x):
    count = lax.axis_size("groups")
    return lax.ppermute(x, "groups", [(g, g ^ 1) for g in range(count)])


def tokens_by_features(span_tokens, depth):
    xs, zs = (lax.axis_size(a) for a in ("x", "z"))
    tokens = span_tokens.shape[0]
    group, x, core = (lax.axis_index(a) for a in ("groups", "x", "width"))
    odd = (group & 1) == 1
    pieces = halves_of_blocks(span_tokens, zs)
    received = with_neighbour(jnp.where(odd, pieces[0], pieces[1]))
    both = jnp.stack([jnp.where(odd, pieces[1], pieces[0]), received], axis=1)
    both = swapped_if((x & 1) == 1, both, 0)
    mine = []
    for i in range(2):
        pairs = []
        for a in range(xs):
            for w in range(2):
                pairs.append((a * 2 + w, (2 * w + ((a & 1) ^ i)) * 2 + (a >> 1)))
        mine.append(lax.ppermute(both[i], ("x", "width"), pairs))
    mine = jnp.stack(mine)
    theirs = lax.ppermute(mine, "width", [(0, 1), (1, 0)])
    ready = jnp.stack([mine, theirs])
    return swapped_if((core ^ (x >> 1)) == 1, ready, 0).reshape(xs, 2, tokens, depth)


def own_half(place, kv_weight):
    rows, width = kv_weight.shape
    half = rows // 2

    def body(place_ref, weight_hbm, out_ref, sem):
        begin = pl.multiple_of((place_ref[3] & 1) * half, half)
        copy = pltpu.make_async_copy(weight_hbm.at[pl.ds(begin, half), :], out_ref, sem)
        copy.start()
        copy.wait()

    return pl.pallas_call(
        body,
        in_specs=[
            pl.BlockSpec(memory_space=pltpu.SMEM),
            pl.BlockSpec(memory_space=pltpu.HBM),
        ],
        out_shape=pltpu.VMEM((half, width), BF16),
        scratch_shapes=[pltpu.SemaphoreType.DMA],
        compiler_params=pltpu.CompilerParams(vmem_limit_bytes=16 * 2**20),
        name="own_half",
    )(place, pltpu.with_memory_space_constraint(kv_weight, pltpu.HBM))


def gathered_over_z(own):
    zs = lax.axis_size("z")
    up = [(i, (i + 1) % zs) for i in range(zs)]
    down = [(i, (i - 1) % zs) for i in range(zs)]
    below = above = own
    blocks = [own]
    for s in range(1, zs // 2 + 1):
        below = lax.ppermute(below, "z", up)
        blocks.append(below)
        if s < zs // 2:
            above = lax.ppermute(above, "z", down)
            blocks.append(above)
    return blocks


def span_dot(place, ready, blocks):
    xs, groups, tokens, depth = ready.shape
    zs = len(blocks)
    block, width = blocks[0].shape
    offsets = [0]
    for s in range(1, zs // 2 + 1):
        offsets += [zs - s, s]
    offsets = offsets[:zs]

    def body(place_ref, ready_ref, *refs):
        home_ref, away_ref = refs[zs:]

        def features(i):
            begin = lax.rem(place_ref[2] + offsets[i], zs) * block
            return ready_ref[:, pl.ds(pl.multiple_of(begin, block), block)]

        total = None
        for i in range(0, zs, 2):
            left = jnp.concatenate([features(i), features(i + 1)], axis=1)
            right = jnp.concatenate([refs[i][...], refs[i + 1][...]], axis=0)
            more = dot_f32(left, right)
            total = more if total is None else total + more
        for m in range(xs):
            begin = m * groups * tokens
            home_ref[m] = total[begin : begin + tokens]
            away_ref[m] = total[begin + tokens : begin + 2 * tokens]

    flat = ready.reshape(xs * groups * tokens, depth)
    outs = [array((xs, tokens, width), F32)] * 2
    return on_chip(body, outs, flat, *blocks, place=place)


def added_at_home(home, away):
    received = with_neighbour(away)
    count = home.shape[0]

    def body(home_ref, received_ref, *outs):
        for m in range(count):
            outs[m][...] = home_ref[m] + received_ref[m]

    outs = [array(home.shape[1:], F32)] * count
    received = exchanged_over_x(on_chip(body, outs, home, received))
    total = received[0]
    for more in received[1:]:
        total = total + more
    return total.astype(BF16)


def biases(lengths, offset, step_count, slots, span):
    branch_count = lengths.shape[0]
    rows = step_count * branch_count
    seat = lax.axis_index(SEQ)
    visible = jnp.tile(jnp.minimum(lengths, offset[0]), step_count)[:, None]
    places = seat * slots + jnp.arange(slots, dtype=jnp.int32)[None]
    row = jnp.arange(rows, dtype=jnp.int32)
    same = (row[:, None] % branch_count == row[None] % branch_count) & (row[None] <= row[:, None])
    every = jnp.ones((rows, span), jnp.bool_)
    filler = jnp.zeros((rows, -(slots + span + rows) % HD), jnp.bool_)
    allowed = jnp.concatenate([places < visible, every, same & (seat == 0), filler], axis=1)
    return jnp.where(allowed, 0.0, MASKED_SCORE).astype(F32)


def local(
    span_tokens,
    kv_weight,
    query_weight,
    out_weight,
    cache_keys,
    cache_values,
    hidden,
    lengths,
    offset,
):
    xs = lax.axis_size("x")
    zs = lax.axis_size("z")
    step_count, branch_count, depth = hidden.shape
    rows = step_count * branch_count
    scale = LOG2E / math.sqrt(HD)
    tokens = span_tokens.shape[0]
    place = jnp.stack([lax.axis_index(a) for a in ("x", "width", "z", "groups")])
    blocks = gathered_over_z(own_half(place, kv_weight))
    partial = project(place, hidden.reshape(rows, depth), query_weight, kv_weight, xs)
    partial = exchanged_over_x(partial)
    ready = tokens_by_features(span_tokens, zs * blocks[0].shape[0])
    partial = add_over_x(partial, zs)
    partial = exchanged(partial, "z")
    own = add_over_z(partial)
    own = exchanged(own, "z")
    span_kv = added_at_home(*span_dot(place, ready, blocks))
    columns = fan(own, rows, HD)
    projected = exchanged_over_x([columns] * xs)

    bias = biases(lengths, offset, step_count, cache_keys.shape[0], tokens)
    keys = cache_keys.transpose(1, 0, 2)
    values = cache_values.transpose(1, 0, 2)
    partial = attend(place, projected, keys, values, span_kv, bias, scale)
    folded = fold(exchanged_over_x(partial), zs)
    ours = finish(exchanged(folded, "z"))
    columns = fan(exchanged(ours, "z"), rows, 0)
    attention = exchanged_over_x([columns] * xs)
    keep, send = close(place, attention, out_weight)
    attended = (keep + lax.ppermute(send, "width", [(0, 1), (1, 0)])).astype(BF16)
    return (span_kv, attended.reshape(step_count, branch_count, attended.shape[1]))


def solution(mesh):
    finer = Mesh(
        mesh.devices.reshape(mesh.shape["groups"], 4, 16, mesh.shape["width"]),
        ("groups", "x", "z", "width"),
    )
    placed = (
        P(GROUPS_SEQ, "width"),
        P(SEQ, "width"),
        P(SEQ, "width"),
        P("width", SEQ),
        P(GROUPS_SEQ, "width", None),
        P(GROUPS_SEQ, "width", None),
        P(None, "groups", SEQ),
        P("groups"),
        P("groups"),
    )

    return jax.shard_map(
        local,
        mesh=finer,
        in_specs=placed,
        out_specs=(P(GROUPS_SEQ, "width"), P(None, "groups", SEQ_WIDTH)),
        check_vma=False,
    )
```

```python
import math

import jax
import jax.numpy as jnp
from jax import lax
from jax.experimental import pallas as pl
from jax.experimental.pallas import tpu as pltpu
from jax.sharding import Mesh
from jax.sharding import PartitionSpec as P


HD = 128
SEQ = ("x", "z")
GROUPS_SEQ = ("groups", *SEQ)
SEQ_WIDTH = (*SEQ, "width")
MASKED_SCORE = -1e30
LOG2E = 1.4426950408889634
F32 = jnp.float32
BF16 = jnp.bfloat16
TILE = 8


def exchanged(pieces, axis):
    return lax.all_to_all(pieces, axis, split_axis=0, concat_axis=0, tiled=True)


def dot_f32(a, b):
    return jnp.dot(a, b, preferred_element_type=F32)


def on_chip(body, outs, *operands, scratch=(), place=None):
    shapes = jax.tree.map(lambda o: pltpu.VMEM(o.shape, o.dtype), outs)
    placed = [pltpu.with_memory_space_constraint(x, pltpu.VMEM) for x in operands]
    specs = [pl.BlockSpec(memory_space=pltpu.VMEM)] * len(placed)
    if place is not None:
        placed.insert(0, place)
        specs.insert(0, pl.BlockSpec(memory_space=pltpu.SMEM))
    params = pltpu.CompilerParams(vmem_limit_bytes=16 * 2**20)
    return pl.pallas_call(
        body, in_specs=specs, out_shape=shapes, scratch_shapes=scratch, compiler_params=params
    )(*placed)


def exchanged_over_x(pieces):
    count = lax.axis_size("x")
    received = [pieces[0]]
    for mask in range(1, count):
        pairs = [(i, i ^ mask) for i in range(count)]
        received.append(lax.ppermute(pieces[mask], "x", pairs))
    return received


def array(shape, dtype):
    return jax.ShapeDtypeStruct(shape, dtype)


def parts_of(rows, places):
    return places // (rows // TILE)


def project(place, states, query_weight, kv_weight, pieces):
    rows, depth = states.shape
    columns = query_weight.shape[1] // pieces
    extra = kv_weight.shape[1] // pieces

    def body(place_ref, states_hbm, query_hbm, fresh_hbm, *rest):
        outs = rest[:pieces]
        states_ref, query_ref, fresh_ref, sems = rest[pieces:]
        x = place_ref[0]
        copies = [pltpu.make_async_copy(states_hbm, states_ref, sems.at[2 * pieces])]
        for m in range(pieces):
            c = x ^ m
            more = fresh_hbm.at[:, pl.ds(pl.multiple_of(c * extra, extra), extra)]
            most = query_hbm.at[:, pl.ds(pl.multiple_of(c * columns, columns), columns)]
            copies.append(pltpu.make_async_copy(more, fresh_ref.at[m], sems.at[2 * m]))
            copies.append(pltpu.make_async_copy(most, query_ref.at[m], sems.at[2 * m + 1]))
        for copy in copies:
            copy.start()
        copies[0].wait()
        states = states_ref[...]
        for m in range(pieces):
            copies[1 + 2 * m].wait()
            outs[m][:, columns:] = dot_f32(states, fresh_ref[m])
            copies[2 + 2 * m].wait()
            outs[m][:, :columns] = dot_f32(states, query_ref[m])

    hbm = [pltpu.with_memory_space_constraint(x, pltpu.HBM) for x in (states, query_weight, kv_weight)]
    return pl.pallas_call(
        body,
        in_specs=[pl.BlockSpec(memory_space=pltpu.SMEM)]
        + [pl.BlockSpec(memory_space=pltpu.HBM)] * len(hbm),
        out_shape=[pltpu.VMEM((rows, columns + extra), F32)] * pieces,
        scratch_shapes=[
            pltpu.VMEM(states.shape, BF16),
            pltpu.VMEM((pieces, depth, columns), BF16),
            pltpu.VMEM((pieces, depth, extra), BF16),
            pltpu.SemaphoreType.DMA((2 * pieces + 1,)),
        ],
        compiler_params=pltpu.CompilerParams(vmem_limit_bytes=16 * 2**20),
        name="project",
    )(place, *hbm)


def add_over_x(received, places):
    rows, width = received[0].shape
    parts = parts_of(rows, places)
    columns = (width - HD) // parts

    def body(*refs):
        out_ref = refs[-1]
        total = refs[0][...]
        for ref in refs[1:-1]:
            total = total + ref[...]
        for part in range(parts):
            for group in range(rows // TILE):
                place = part * (rows // TILE) + group
                some = total[group * TILE : (group + 1) * TILE]
                out_ref[place, :, :columns] = some[:, part * columns : (part + 1) * columns]
                out_ref[place, :, columns:] = some[:, width - HD :]

    return on_chip(body, array((places, TILE, columns + HD), F32), *received)


def add_over_z(received):
    def body(in_ref, out_ref):
        total = in_ref[0]
        for s in range(1, in_ref.shape[0]):
            total = total + in_ref[s]
        total = total.astype(BF16)
        for s in range(in_ref.shape[0]):
            out_ref[s] = total

    return on_chip(body, array(received.shape, BF16), received)


def fan(received, rows, tail):
    places, _, width = received.shape
    parts = parts_of(rows, places)
    columns = width - tail
    whole = parts * columns + tail

    def body(in_ref, out_ref):
        for part in range(parts):
            for pair in range(rows // TILE // 2):
                place = part * (rows // TILE) + 2 * pair
                some = jnp.concatenate(
                    [in_ref[place].astype(F32), in_ref[place + 1].astype(F32)], axis=0
                ).astype(BF16)
                at = slice(2 * pair * TILE, 2 * (pair + 1) * TILE)
                out_ref[at, part * columns : (part + 1) * columns] = some[:, :columns]
                if tail and part == 0:
                    out_ref[at, parts * columns :] = some[:, columns:]

    return on_chip(body, array((rows, whole), BF16), received)


def three_parts(x):
    high = x.astype(BF16).astype(F32)
    rest = x - high
    middle = rest.astype(BF16).astype(F32)
    return (high, middle, rest - middle)


def joined_stats(tail, heads):
    lanes = tail.shape[-1]
    whole = tail + pltpu.roll(tail, lanes - heads, 1) + pltpu.roll(tail, lanes - 2 * heads, 1)
    return whole, pltpu.roll(whole, lanes - 3 * heads, 1)


def split_stats(highest, total, heads):
    lane = lax.broadcasted_iota(jnp.int32, highest.shape, 1)
    parts = (*three_parts(highest), *three_parts(total))
    stats = jnp.where(lane < heads, parts[0], 0.0)
    for place in range(1, 6):
        here = (lane >= place * heads) & (lane < (place + 1) * heads)
        stats = jnp.where(here, pltpu.roll(parts[place], place * heads, 1), stats)
    return stats


def heads_together(ref, first, count):
    return jnp.concatenate(
        [ref[:, (first + i) * HD : (first + i + 1) * HD] for i in range(count)], axis=0
    )


def score(q, keys):
    return lax.dot_general(q, keys, (((1,), (1,)), ((), ())), preferred_element_type=F32)


def attend(place, projected, keys, values, span_kv, bias, scale):
    pieces = len(projected)
    rows, width = projected[0].shape
    local_heads, slots, _ = keys.shape
    span = span_kv.shape[0]
    per_head = pieces // local_heads
    total_keys = bias.shape[1]
    heads = (width - HD) // HD
    per_dot = 256 // rows
    at = heads * HD
    blank_rows = total_keys - slots - rows - span

    def body(place_ref, *refs):
        q_refs = refs[:pieces]
        keys_ref, values_ref, span_ref, bias_ref = refs[pieces : pieces + 4]
        outs = refs[pieces + 4 : 2 * pieces + 4]
        k_ref, v_ref = refs[2 * pieces + 4 :]
        x = place_ref[0]
        odd = (x & 1) == 1
        bias = bias_ref[...]
        lane = lax.broadcasted_iota(jnp.int32, (rows, HD), 1)
        blank = [jnp.zeros((blank_rows, HD), BF16)] if blank_rows else []
        for h in range(local_heads):
            head = (x >> 1) ^ h
            k_ref[h, :slots, :] = keys_ref[head]
            v_ref[h, :slots, :] = values_ref[head]
            first = q_refs[h * per_head][:, at:].astype(F32)
            second = q_refs[h * per_head + 1][:, at:].astype(F32)
            fresh = (jnp.where(odd, second, first), jnp.where(odd, first, second))
            for side, into in enumerate((k_ref, v_ref)):
                begin = pl.multiple_of((2 * head + side) * HD, HD)
                more = [span_ref[:, pl.ds(begin, HD)], fresh[side].astype(BF16)]
                into[h, slots:, :] = jnp.concatenate(more + blank, axis=0)
        for piece in range(pieces):
            h = piece // per_head
            peaks = jnp.zeros((rows, HD), F32)
            totals = jnp.zeros((rows, HD), F32)
            for first in range(0, heads, per_dot):
                q = heads_together(q_refs[piece], first, per_dot)
                scores = score(q, k_ref[h])
                scores = scores.reshape(per_dot, rows, total_keys) * scale + bias[None]
                highest = jnp.max(scores, axis=-1, keepdims=True)
                weights = jnp.exp2(scores - highest)
                total = jnp.sum(weights, axis=-1, keepdims=True)
                weights = weights.reshape(per_dot * rows, total_keys).astype(BF16)
                summed = dot_f32(weights, v_ref[h])
                for i in range(per_dot):
                    head = first + i
                    outs[piece][:, head * HD : (head + 1) * HD] = summed[
                        i * rows : (i + 1) * rows
                    ].astype(BF16)
                    peaks = jnp.where(lane == head, highest[i], peaks)
                    totals = jnp.where(lane == head, total[i], totals)
            outs[piece][:, at:] = split_stats(peaks, totals, heads).astype(BF16)

    out = [array((rows, width), BF16)] * pieces
    scratch = [pltpu.VMEM((local_heads, total_keys, HD), BF16)] * 2
    operands = (*projected, keys, values, span_kv, bias)
    return on_chip(body, out, *operands, scratch=scratch, place=place)


def fold(received, places):
    sources = len(received)
    rows, width = received[0].shape
    heads = (width - HD) // HD
    at = heads * HD
    parts = parts_of(rows, places)
    some_heads = heads // parts
    groups = rows // TILE
    columns = some_heads * HD

    def body(*refs):
        out_ref = refs[-1]
        lane = lax.broadcasted_iota(jnp.int32, (rows, HD), 1)
        stats = [joined_stats(refs[s][:, at:].astype(F32), heads) for s in range(sources)]
        highest = stats[0][0]
        for s in range(1, sources):
            highest = jnp.maximum(highest, stats[s][0])
        keeps = [jnp.exp2(jnp.where(lane < heads, m - highest, 0.0)) for m, _ in stats]
        total = keeps[0] * stats[0][1]
        for s in range(1, sources):
            total = total + keeps[s] * stats[s][1]

        def put(part, cut, block):
            for group in range(groups):
                out_ref[part * groups + group, :, cut] = block[
                    group * TILE : (group + 1) * TILE
                ].astype(BF16)

        for part in range(parts):
            for i in range(some_heads):
                head = part * some_heads + i
                cut = slice(head * HD, (head + 1) * HD)
                summed = refs[0][:, cut].astype(F32) * keeps[0][:, head : head + 1]
                for s in range(1, sources):
                    keep = keeps[s][:, head : head + 1]
                    summed = summed + refs[s][:, cut].astype(F32) * keep
                put(part, slice(i * HD, (i + 1) * HD), summed)
            turn = (HD - part * some_heads) % HD
            peaks = pltpu.roll(highest, turn, 1) if turn else highest
            totals = pltpu.roll(total, turn, 1) if turn else total
            put(part, slice(columns, columns + HD), split_stats(peaks, totals, some_heads))

    return on_chip(body, array((places, TILE, columns + HD), BF16), *received)


def finish(received):
    sources, group, width = received.shape
    heads = (width - HD) // HD
    at = heads * HD

    def body(in_ref, out_ref):
        lane = lax.broadcasted_iota(jnp.int32, (group, HD), 1)
        stats = [joined_stats(in_ref[s, :, at:].astype(F32), heads) for s in range(sources)]
        highest = stats[0][0]
        for s in range(1, sources):
            highest = jnp.maximum(highest, stats[s][0])
        keeps = [jnp.exp2(jnp.where(lane < heads, m - highest, 0.0)) for m, _ in stats]
        total = keeps[0] * stats[0][1]
        for s in range(1, sources):
            total = total + keeps[s] * stats[s][1]
        for head in range(heads):
            cut = slice(head * HD, (head + 1) * HD)
            summed = in_ref[0, :, cut].astype(F32) * keeps[0][:, head : head + 1]
            for s in range(1, sources):
                summed = summed + in_ref[s, :, cut].astype(F32) * keeps[s][:, head : head + 1]
            ready = (summed / total[:, head : head + 1]).astype(BF16)
            for s in range(sources):
                out_ref[s, :, cut] = ready

    return on_chip(body, array((sources, group, at), BF16), received)


def close(place, attention, out_weight):
    pieces = len(attention)
    rows, depth = attention[0].shape
    columns = out_weight.shape[1] // 2

    def body(place_ref, *refs):
        weight_ref, keep_ref, send_ref = refs[pieces:]
        total = None
        for m in range(pieces):
            begin = pl.multiple_of((place_ref[0] ^ m) * depth, depth)
            more = dot_f32(refs[m][...], weight_ref[pl.ds(begin, depth), :])
            total = more if total is None else total + more
        upper = place_ref[1] == 1
        left, right = total[:, :columns], total[:, columns:]
        keep_ref[...] = jnp.where(upper, right, left)
        send_ref[...] = jnp.where(upper, left, right)

    outs = [array((rows, columns), F32)] * 2
    return on_chip(body, outs, *attention, out_weight, place=place)


def halves_of_blocks(place, span_tokens, places):
    tokens, width = span_tokens.shape
    block = width // (4 * places)

    def body(place_ref, in_ref, own_ref, other_ref):
        odd = place_ref[3] & 1
        for k in range(2):
            for spot in range(places):
                first = (k * places + spot) * 2
                cut = slice(spot * block, (spot + 1) * block)
                for out_ref, half in ((own_ref, odd), (other_ref, 1 - odd)):
                    begin = pl.multiple_of((first + half) * block, block)
                    out_ref[k, :, cut] = in_ref[:, pl.ds(begin, block)]

    outs = [array((2, tokens, places * block), BF16)] * 2
    return on_chip(body, outs, span_tokens, place=place)


def by_parity(place, own, received):
    _, tokens, depth = own.shape

    def body(place_ref, own_ref, received_ref, *outs):
        for i in range(2):
            k = (place_ref[0] & 1) ^ i
            outs[i][0] = own_ref[k]
            outs[i][1] = received_ref[k]

    outs = [array((2, tokens, depth), BF16)] * 2
    return on_chip(body, outs, own, received, place=place)


def with_neighbour(x):
    count = lax.axis_size("groups")
    return lax.ppermute(x, "groups", [(g, g ^ 1) for g in range(count)])


def tokens_by_features(place, span_tokens):
    xs, zs = (lax.axis_size(a) for a in ("x", "z"))
    own, other = halves_of_blocks(place, span_tokens, zs)
    received = with_neighbour(other)
    mine = []
    for i, piece in enumerate(by_parity(place, own, received)):
        pairs = []
        for a in range(xs):
            for w in range(2):
                pairs.append((a * 2 + w, (2 * w + ((a & 1) ^ i)) * 2 + (a >> 1)))
        mine.append(lax.ppermute(piece, ("x", "width"), pairs))
    theirs = []
    for i in range(2):
        theirs.append(lax.ppermute(mine[i], "width", [(0, 1), (1, 0)]))
    return mine + theirs


def own_half(place, kv_weight):
    rows, width = kv_weight.shape
    half = rows // 2

    def body(place_ref, weight_hbm, out_ref, sem):
        begin = pl.multiple_of((place_ref[3] & 1) * half, half)
        copy = pltpu.make_async_copy(weight_hbm.at[pl.ds(begin, half), :], out_ref, sem)
        copy.start()
        copy.wait()

    return pl.pallas_call(
        body,
        in_specs=[
            pl.BlockSpec(memory_space=pltpu.SMEM),
            pl.BlockSpec(memory_space=pltpu.HBM),
        ],
        out_shape=pltpu.VMEM((half, width), BF16),
        scratch_shapes=[pltpu.SemaphoreType.DMA],
        compiler_params=pltpu.CompilerParams(vmem_limit_bytes=16 * 2**20),
        name="own_half",
    )(place, pltpu.with_memory_space_constraint(kv_weight, pltpu.HBM))


def gathered_over_z(own):
    zs = lax.axis_size("z")
    up = [(i, (i + 1) % zs) for i in range(zs)]
    down = [(i, (i - 1) % zs) for i in range(zs)]
    below = above = own
    blocks = [own]
    for s in range(1, zs // 2 + 1):
        below = lax.ppermute(below, "z", up)
        blocks.append(below)
        if s < zs // 2:
            above = lax.ppermute(above, "z", down)
            blocks.append(above)
    return blocks


def span_dot(place, ready, blocks):
    groups, tokens, _ = ready[0].shape
    count = len(ready)
    zs = len(blocks)
    block, width = blocks[0].shape
    offsets = [0]
    for s in range(1, zs // 2 + 1):
        offsets += [zs - s, s]
    offsets = offsets[:zs]

    def body(place_ref, *refs):
        tokens_refs = refs[:count]
        block_refs = refs[count : count + zs]
        home_ref, away_ref = refs[count + zs :]

        def features(i):
            begin = lax.rem(place_ref[2] + offsets[i], zs) * block
            cut = pl.ds(pl.multiple_of(begin, block), block)
            return jnp.concatenate(
                [ref[o, :, cut] for ref in tokens_refs for o in range(groups)], axis=0
            )

        total = None
        for i in range(0, zs, 2):
            left = jnp.concatenate([features(i), features(i + 1)], axis=1)
            right = jnp.concatenate([block_refs[i][...], block_refs[i + 1][...]], axis=0)
            more = dot_f32(left, right)
            total = more if total is None else total + more
        turned = place_ref[1] ^ (place_ref[0] >> 1)
        for n in range(count):
            m = 2 * ((n >> 1) ^ turned) + (n & 1)
            begin = n * groups * tokens
            home_ref[m] = total[begin : begin + tokens]
            away_ref[m] = total[begin + tokens : begin + 2 * tokens]

    outs = [array((count, tokens, width), F32)] * 2
    return on_chip(body, outs, *ready, *blocks, place=place)


def added_at_home(home, away):
    received = with_neighbour(away)
    count = home.shape[0]

    def body(home_ref, received_ref, *outs):
        for m in range(count):
            outs[m][...] = home_ref[m] + received_ref[m]

    outs = [array(home.shape[1:], F32)] * count
    received = exchanged_over_x(on_chip(body, outs, home, received))
    total = received[0]
    for more in received[1:]:
        total = total + more
    return total.astype(BF16)


def biases(lengths, offset, step_count, slots, span):
    branch_count = lengths.shape[0]
    rows = step_count * branch_count
    seat = lax.axis_index(SEQ)
    visible = jnp.tile(jnp.minimum(lengths, offset[0]), step_count)[:, None]
    places = seat * slots + jnp.arange(slots, dtype=jnp.int32)[None]
    row = jnp.arange(rows, dtype=jnp.int32)
    same = (row[:, None] % branch_count == row[None] % branch_count) & (row[None] <= row[:, None])
    every = jnp.ones((rows, span), jnp.bool_)
    filler = jnp.zeros((rows, -(slots + span + rows) % HD), jnp.bool_)
    allowed = jnp.concatenate([places < visible, every, same & (seat == 0), filler], axis=1)
    return jnp.where(allowed, 0.0, MASKED_SCORE).astype(F32)


def local(
    span_tokens,
    kv_weight,
    query_weight,
    out_weight,
    cache_keys,
    cache_values,
    hidden,
    lengths,
    offset,
):
    xs = lax.axis_size("x")
    zs = lax.axis_size("z")
    step_count, branch_count, depth = hidden.shape
    rows = step_count * branch_count
    scale = LOG2E / math.sqrt(HD)
    tokens = span_tokens.shape[0]
    place = jnp.stack([lax.axis_index(a) for a in ("x", "width", "z", "groups")])
    blocks = gathered_over_z(own_half(place, kv_weight))
    partial = project(place, hidden.reshape(rows, depth), query_weight, kv_weight, xs)
    partial = exchanged_over_x(partial)
    ready = tokens_by_features(place, span_tokens)
    partial = add_over_x(partial, zs)
    partial = exchanged(partial, "z")
    own = add_over_z(partial)
    own = exchanged(own, "z")
    span_kv = added_at_home(*span_dot(place, ready, blocks))
    columns = fan(own, rows, HD)
    projected = exchanged_over_x([columns] * xs)

    bias = biases(lengths, offset, step_count, cache_keys.shape[0], tokens)
    keys = cache_keys.transpose(1, 0, 2)
    values = cache_values.transpose(1, 0, 2)
    partial = attend(place, projected, keys, values, span_kv, bias, scale)
    folded = fold(exchanged_over_x(partial), zs)
    ours = finish(exchanged(folded, "z"))
    columns = fan(exchanged(ours, "z"), rows, 0)
    attention = exchanged_over_x([columns] * xs)
    keep, send = close(place, attention, out_weight)
    attended = (keep + lax.ppermute(send, "width", [(0, 1), (1, 0)])).astype(BF16)
    return (span_kv, attended.reshape(step_count, branch_count, attended.shape[1]))


def solution(mesh):
    finer = Mesh(
        mesh.devices.reshape(mesh.shape["groups"], 4, 16, mesh.shape["width"]),
        ("groups", "x", "z", "width"),
    )
    placed = (
        P(GROUPS_SEQ, "width"),
        P(SEQ, "width"),
        P(SEQ, "width"),
        P("width", SEQ),
        P(GROUPS_SEQ, "width", None),
        P(GROUPS_SEQ, "width", None),
        P(None, "groups", SEQ),
        P("groups"),
        P("groups"),
    )

    return jax.shard_map(
        local,
        mesh=finer,
        in_specs=placed,
        out_specs=(P(GROUPS_SEQ, "width"), P(None, "groups", SEQ_WIDTH)),
        check_vma=False,
    )
```
